16 devices in a mesh: dp: 4 (over z, y), ep: 4 (over x, core).
Axes of the slice: x: 2, y: 2, z: 2, core: 2. Of those that a mesh axis runs over, the one named last changes fastest.
Arguments:
- tokens: bfloat16 [4096, 1024], P(('dp', 'ep'))
- w_router: bfloat16 [1024, 32], replicated
- w_gate: bfloat16 [32, 1024, 512], P('ep')
- w_up: bfloat16 [32, 1024, 512], P('ep')
- w_down: bfloat16 [32, 512, 1024], P('ep')
- top_ids: int32 [4096, 8], P(('dp', 'ep'))
- r_proj: bfloat16 [4096, 1024], P(('dp', 'ep'))
Outputs:
- output 1: float32 [4096, 1024], P(('dp', 'ep'))
- output 2: float32 [4096, 1024], P(('dp', 'ep'))
- output 3: float32 [32, 1024, 512], P('ep')
- output 4: float32 [32, 1024, 512], P('ep')
- output 5: float32 [32, 512, 1024], P('ep')
- output 6: float32 [1024, 32], replicated
All inputs are finite; a program needn't handle non-finite values.
Results may differ from the reference program's by a relative error of at most 0.00174.
Values are sent between devices in bfloat16 or wider.
A program may use at most 1 GiB of HBM per device.

```python
import jax
import jax.numpy as jnp
from jax import lax

D = 1024
FF = 512
EXPERTS = 32
TOP = 8
N_TOK = 4096
BLK = 64
ASSIGN = N_TOK * TOP
NBLK = (ASSIGN + BLK - 1) // BLK + EXPERTS
ROWS = NBLK * BLK


def draw_routing(rng_key):
    key_rank, key_noise = jax.random.split(rng_key)
    expert_rank = jax.random.permutation(key_rank, EXPERTS)
    popular = 2000 // (expert_rank + 2)
    rand_noise = jax.random.randint(key_noise, (N_TOK, EXPERTS), 0, 1000)
    int_score = (popular[None, :] + rand_noise) * EXPERTS + jnp.arange(EXPERTS)[None, :]
    return lax.top_k(int_score, TOP)[1].astype(jnp.int32)


def setup_inputs(seed: int = 0) -> dict:
    key_list = jax.random.split(jax.random.key(seed), 7)
    tokens = jax.random.normal(key_list[0], (N_TOK, D), jnp.float32).astype(jnp.bfloat16)
    w_router = (jax.random.normal(key_list[1], (D, EXPERTS), jnp.float32) * D ** -0.5).astype(jnp.bfloat16)
    w_gate = (jax.random.normal(key_list[2], (EXPERTS, D, FF), jnp.float32) * D ** -0.5).astype(jnp.bfloat16)
    w_up = (jax.random.normal(key_list[3], (EXPERTS, D, FF), jnp.float32) * D ** -0.5).astype(jnp.bfloat16)
    w_down = (jax.random.normal(key_list[4], (EXPERTS, FF, D), jnp.float32) * FF ** -0.5).astype(jnp.bfloat16)
    top_ids = draw_routing(key_list[5])
    r_proj = jax.random.normal(key_list[6], (N_TOK, D), jnp.float32).astype(jnp.bfloat16)
    return {'tokens': tokens, 'w_router': w_router, 'w_gate': w_gate, 'w_up': w_up, 'w_down': w_down, 'top_ids': top_ids, 'r_proj': r_proj}


def reference(tokens, w_router, w_gate, w_up, w_down, top_ids, r_proj):
    logits = jnp.dot(tokens, w_router, preferred_element_type=jnp.float32)
    gate_prob = jax.nn.softmax(jnp.take_along_axis(logits, top_ids, axis=1), axis=-1)
    exp_flat = top_ids.reshape(-1)
    sort_idx = jnp.argsort(exp_flat, stable=True).astype(jnp.int32)
    sorted_exp = exp_flat[sort_idx]
    exp_count = jnp.bincount(exp_flat, length=EXPERTS).astype(jnp.int32)
    pad_count = (exp_count + BLK - 1) // BLK * BLK
    pad_end = jnp.cumsum(pad_count)
    pad_start = pad_end - pad_count
    cnt_start = jnp.cumsum(exp_count) - exp_count
    row_pos = pad_start[sorted_exp] + jnp.arange(ASSIGN, dtype=jnp.int32) - cnt_start[sorted_exp]
    slot_asg = jnp.full((ROWS,), ASSIGN, jnp.int32).at[row_pos].set(sort_idx)
    pos_asg = jnp.zeros((ASSIGN,), jnp.int32).at[sort_idx].set(row_pos)
    blk_start = jnp.arange(NBLK, dtype=jnp.int32) * BLK
    blk_exp = jnp.minimum(jnp.sum((pad_end[None, :] <= blk_start[:, None]).astype(jnp.int32), axis=1), EXPERTS - 1)
    row_valid = (slot_asg < ASSIGN)[:, None]
    safe_asg = jnp.minimum(slot_asg, ASSIGN - 1)
    tok_rows = jnp.where(row_valid, tokens[safe_asg // TOP], 0).reshape(NBLK, BLK, D)
    contract_rows = (((0,), (0,)), ((), ()))
    contract_cols = (((1,), (1,)), ((), ()))

    def fwd_block(blk_args):
        x_blk, expert = blk_args
        h_gate = jnp.dot(x_blk, w_gate[expert], preferred_element_type=jnp.float32)
        h_up = jnp.dot(x_blk, w_up[expert], preferred_element_type=jnp.float32)
        act_rows = (jax.nn.silu(h_gate) * h_up).astype(jnp.bfloat16)
        return jnp.dot(act_rows, w_down[expert], preferred_element_type=jnp.float32).astype(jnp.bfloat16)

    out_pad = lax.map(fwd_block, (tok_rows, blk_exp)).reshape(ROWS, D)
    out_asg = out_pad[pos_asg].reshape(N_TOK, TOP, D).astype(jnp.float32)
    y_out = tokens.astype(jnp.float32) + jnp.einsum('tkh,tk->th', out_asg, gate_prob)

    d_y = r_proj.astype(jnp.float32)
    d_gates = jnp.einsum('tkh,th->tk', out_asg, d_y)
    d_sel = gate_prob * (d_gates - jnp.sum(gate_prob * d_gates, axis=-1, keepdims=True))
    onehot = (top_ids[:, :, None] == jnp.arange(EXPERTS)[None, None, :]).astype(jnp.float32)
    d_logit = jnp.einsum('tk,tke->te', d_sel, onehot).astype(jnp.bfloat16)
    grad_router = lax.dot_general(tokens, d_logit, contract_rows, preferred_element_type=jnp.float32)
    dx_router = lax.dot_general(d_logit, w_router, contract_cols, preferred_element_type=jnp.float32)
    d_out = (gate_prob[:, :, None] * d_y[:, None, :]).astype(jnp.bfloat16).reshape(ASSIGN, D)
    d_pad = jnp.where(row_valid, d_out[safe_asg], 0).reshape(NBLK, BLK, D)

    def bwd_block(grad_acc, blk_args):
        g_gate, g_up, g_down = grad_acc
        x_blk, d_blk, expert = blk_args
        h_gate = jnp.dot(x_blk, w_gate[expert], preferred_element_type=jnp.float32)
        h_up = jnp.dot(x_blk, w_up[expert], preferred_element_type=jnp.float32)
        sig_gate = jax.nn.sigmoid(h_gate)
        silu_gate = h_gate * sig_gate
        act_rows = (silu_gate * h_up).astype(jnp.bfloat16)
        d_act = lax.dot_general(d_blk, w_down[expert], contract_cols, preferred_element_type=jnp.float32)
        d_hgate = (d_act * h_up * sig_gate * (1.0 + h_gate * (1.0 - sig_gate))).astype(jnp.bfloat16)
        d_hup = (d_act * silu_gate).astype(jnp.bfloat16)
        g_gate = g_gate.at[expert].add(lax.dot_general(x_blk, d_hgate, contract_rows, preferred_element_type=jnp.float32))
        g_up = g_up.at[expert].add(lax.dot_general(x_blk, d_hup, contract_rows, preferred_element_type=jnp.float32))
        g_down = g_down.at[expert].add(lax.dot_general(act_rows, d_blk, contract_rows, preferred_element_type=jnp.float32))
        d_rows = lax.dot_general(d_hgate, w_gate[expert], contract_cols, preferred_element_type=jnp.float32) + lax.dot_general(d_hup, w_up[expert], contract_cols, preferred_element_type=jnp.float32)
        return (g_gate, g_up, g_down), d_rows.astype(jnp.bfloat16)

    zero_in = jnp.zeros((EXPERTS, D, FF), jnp.float32)
    zero_out = jnp.zeros((EXPERTS, FF, D), jnp.float32)
    grads, d_rows = lax.scan(bwd_block, (zero_in, zero_in, zero_out), (tok_rows, d_pad, blk_exp))
    d_expert = jnp.sum(d_rows.reshape(ROWS, D)[pos_asg].reshape(N_TOK, TOP, D).astype(jnp.float32), axis=1)
    grad_tokens = d_y + dx_router + d_expert
    return y_out, grad_tokens, grads[0], grads[1], grads[2], grad_router
```

```python
import functools

import jax
import jax.numpy as jnp
from jax import lax
from jax.experimental import pallas as pl
from jax.experimental.pallas import tpu as pltpu
from jax.sharding import PartitionSpec as P

F32 = jnp.float32
BF16 = jnp.bfloat16
GRP = 16
TILE = 256
BLK = 256


def _dot(a, b, ca, cb):
    return lax.dot_general(a, b, (((ca,), (cb,)), ((), ())), preferred_element_type=F32)


def sort_kernel(meta_ref, dst_ref, gt_ref, xr_ref, out_ref, slot_ref, buf_ref, pend_ref, sem_ref, *, n_exp, hidden, n_blk):
    i = pl.program_id(0)

    @pl.when(i == 0)
    def _():
        pend_ref[0] = 0
        pend_ref[1] = 0
        pend_ref[2] = 0

    n_grp = meta_ref[i, n_exp]
    n_step = (n_grp + TILE // GRP - 1) // (TILE // GRP)
    gates_t = gt_ref[0]
    sel = gates_t >= 0.0
    tri = (lax.broadcasted_iota(jnp.int32, (BLK, BLK), 0) < lax.broadcasted_iota(jnp.int32, (BLK, BLK), 1)).astype(F32).astype(BF16)
    pos = _dot(jnp.where(sel, 1.0, 0.0).astype(BF16), tri, 1, 0).astype(jnp.int32)
    row_id = lax.broadcasted_iota(jnp.int32, (n_exp, BLK), 0)
    start = jnp.zeros((n_exp, BLK), jnp.int32)
    for e in range(n_exp):
        start = jnp.where(row_id == e, meta_ref[i, e], start)
    slot_ref[...] = jnp.where(sel, pos + start, -1)

    def drain(s):
        def one(_, c):
            pltpu.make_async_copy(buf_ref.at[0, pl.ds(0, GRP), :], out_ref.at[pl.ds(0, GRP), :], sem_ref.at[s]).wait()
            return c

        lax.fori_loop(0, pend_ref[s], one, 0)

    def step(k, c):
        s = lax.rem(pend_ref[2], 2)
        pend_ref[2] = pend_ref[2] + 1
        ids = lax.broadcasted_iota(jnp.int32, (TILE, BLK), 0) + k * TILE
        hot = jnp.zeros((TILE, BLK), F32)
        gsel = jnp.zeros((TILE, BLK), F32)
        for e in range(n_exp):
            eq = slot_ref[e : e + 1, :] == ids
            hot = jnp.where(eq, 1.0, hot)
            gsel = jnp.where(eq, gt_ref[0, e : e + 1, :], gsel)
        hot = hot.astype(BF16)
        gcol = jnp.sum(gsel, axis=1, keepdims=True)
        drain(s)
        buf_ref[s, :, :hidden] = _dot(hot, xr_ref[:, :hidden], 1, 0).astype(BF16)
        buf_ref[s, :, hidden:] = (gcol * _dot(hot, xr_ref[:, hidden:], 1, 0)).astype(BF16)
        cnt = jnp.minimum(n_grp - k * (TILE // GRP), TILE // GRP)
        pend_ref[s] = cnt

        def send(q, c):
            dst = pl.multiple_of(dst_ref[i, k * (TILE // GRP) + q], GRP)
            pltpu.make_async_copy(buf_ref.at[s, pl.ds(pl.multiple_of(q * GRP, GRP), GRP), :], out_ref.at[pl.ds(dst, GRP), :], sem_ref.at[s]).start()
            return c

        lax.fori_loop(0, cnt, send, 0)
        return c

    lax.fori_loop(0, n_step, step, 0)

    @pl.when(i == n_blk - 1)
    def _():
        drain(0)
        drain(1)


def sort_rows(meta, dst, gates_t, xr, rot, rows):
    n_blk, n_exp, _ = gates_t.shape
    width = xr.shape[1]
    spec = pltpu.PrefetchScalarGridSpec(
        num_scalar_prefetch=3,
        grid=(n_blk,),
        in_specs=[
            pl.BlockSpec((1, n_exp, BLK), lambda i, m, d, r: (i, 0, 0)),
            pl.BlockSpec((BLK, width), lambda i, m, d, r: (lax.rem(r[0] + i, n_blk), 0)),
        ],
        out_specs=pl.BlockSpec(memory_space=pl.ANY),
        scratch_shapes=[
            pltpu.VMEM((n_exp, BLK), jnp.int32),
            pltpu.VMEM((2, TILE, width), BF16),
            pltpu.SMEM((3,), jnp.int32),
            pltpu.SemaphoreType.DMA((2,)),
        ],
    )

    def kern(m, d, r, *rest):
        sort_kernel(m, d, *rest, n_exp=n_exp, hidden=width // 2, n_blk=n_blk)

    return pl.pallas_call(
        kern,
        out_shape=jax.ShapeDtypeStruct((rows, width), BF16),
        grid_spec=spec,
        name="sort_rows",
        cost_estimate=pl.CostEstimate(flops=20_000_000_000, bytes_accessed=50_000_000, transcendentals=0),
    )(meta, dst, rot, gates_t, xr)


def grouped_kernel(t_ref, ud_ref, w1_ref, w3_ref, w2_ref, o_ref, g1_ref, g3_ref, g2_ref, in_ref, ob_ref, cnt_ref, isem, osem, *, n_exp, hidden):
    e = pl.program_id(0)
    base, valid, n_tile, n_own, first, obase = (t_ref[r, e] for r in range(6))

    def fetch(row, s):
        return pltpu.make_async_copy(ud_ref.at[pl.ds(pl.multiple_of(row, GRP), TILE), :], in_ref.at[s], isem.at[s])

    def put(row, s):
        return pltpu.make_async_copy(ob_ref.at[s], o_ref.at[pl.ds(pl.multiple_of(row, GRP), TILE), :], osem.at[s])

    @pl.when(e == 0)
    def _():
        cnt_ref[0] = 0
        fetch(base, 0).start()

    g1_ref[...] = jnp.zeros_like(g1_ref)
    g3_ref[...] = jnp.zeros_like(g3_ref)
    g2_ref[...] = jnp.zeros_like(g2_ref)

    def tile(k, c):
        s = lax.rem(first + k, 2)
        fetch(base, s).wait()
        last = k == n_tile - 1
        nxt = jnp.where(last, t_ref[0, jnp.minimum(e + 1, n_exp - 1)], base + (k + 1) * TILE)

        @pl.when(jnp.logical_or(jnp.logical_not(last), e < n_exp - 1))
        def _():
            fetch(nxt, 1 - s).start()

        left = valid - k * TILE
        u = in_ref[s, :, :hidden]
        d = in_ref[s, :, hidden:]
        ok = lax.broadcasted_iota(jnp.int32, (TILE, hidden), 0) < left
        u = jnp.where(ok, u, jnp.zeros_like(u))
        d = jnp.where(ok, d, jnp.zeros_like(d))
        h1 = _dot(u, w1_ref[0], 1, 0)
        h3 = _dot(u, w3_ref[0], 1, 0)
        da = _dot(d, w2_ref[0], 1, 1)
        sig = jax.nn.sigmoid(h1)
        silu = h1 * sig
        act = (silu * h3).astype(BF16)
        dh1 = (da * h3 * sig * (1.0 + h1 * (1.0 - sig))).astype(BF16)
        dh3 = (da * silu).astype(BF16)
        g1_ref[0] += _dot(u, dh1, 0, 0)
        g3_ref[0] += _dot(u, dh3, 0, 0)
        g2_ref[0] += _dot(act, d, 0, 0)

        @pl.when(k < n_own)
        def _():
            n = cnt_ref[0]
            cnt_ref[0] = n + 1
            os = lax.rem(n, 2)

            @pl.when(n >= 2)
            def _():
                put(0, os).wait()

            ob_ref[os, :, :hidden] = _dot(act, w2_ref[0], 1, 0).astype(BF16)
            ob_ref[os, :, hidden:] = (_dot(dh1, w1_ref[0], 1, 1) + _dot(dh3, w3_ref[0], 1, 1)).astype(BF16)
            put(obase + k * TILE, os).start()

        return c

    lax.fori_loop(0, n_tile, tile, 0)

    @pl.when(e == n_exp - 1)
    def _():
        n = cnt_ref[0]

        @pl.when(n >= 1)
        def _():
            put(0, lax.rem(n - 1, 2)).wait()

        @pl.when(n >= 2)
        def _():
            put(0, lax.rem(n, 2)).wait()


def grouped(table, ud, w1, w3, w2, own_rows):
    n_exp, hidden, inner = w1.shape
    width = ud.shape[1]
    wspec = lambda a, b: pl.BlockSpec((1, a, b), lambda e, t: (e, 0, 0))
    spec = pltpu.PrefetchScalarGridSpec(
        num_scalar_prefetch=1,
        grid=(n_exp,),
        in_specs=[pl.BlockSpec(memory_space=pl.ANY), wspec(hidden, inner), wspec(hidden, inner), wspec(inner, hidden)],
        out_specs=[pl.BlockSpec(memory_space=pl.ANY), wspec(hidden, inner), wspec(hidden, inner), wspec(inner, hidden)],
        scratch_shapes=[
            pltpu.VMEM((2, TILE, width), BF16),
            pltpu.VMEM((2, TILE, width), BF16),
            pltpu.SMEM((1,), jnp.int32),
            pltpu.SemaphoreType.DMA((2,)),
            pltpu.SemaphoreType.DMA((2,)),
        ],
    )
    return pl.pallas_call(
        functools.partial(grouped_kernel, n_exp=n_exp, hidden=hidden),
        out_shape=[
            jax.ShapeDtypeStruct((own_rows, width), BF16),
            jax.ShapeDtypeStruct(w1.shape, F32),
            jax.ShapeDtypeStruct(w3.shape, F32),
            jax.ShapeDtypeStruct(w2.shape, F32),
        ],
        grid_spec=spec,
        name="grouped",
        compiler_params=pltpu.CompilerParams(vmem_limit_bytes=60 * 1024 * 1024),
        cost_estimate=pl.CostEstimate(flops=60_000_000_000, bytes_accessed=150_000_000, transcendentals=4_000_000),
    )(table, ud, w1, w3, w2)


def combine_kernel(meta_ref, src_ref, g_ref, r_ref, o_ref, y_ref, dx_ref, dg_ref, buf_ref, sem_ref, *, n_exp, hidden):
    i = pl.program_id(0)
    n_grp = meta_ref[i, n_exp]
    n_step = (n_grp + TILE // GRP - 1) // (TILE // GRP)
    full = n_step * (TILE // GRP)

    def pull(q, c):
        src = pl.multiple_of(src_ref[i, q], GRP)
        pltpu.make_async_copy(o_ref.at[pl.ds(src, GRP), :], buf_ref.at[pl.ds(pl.multiple_of(q * GRP, GRP), GRP), :], sem_ref.at[0]).start()
        return c

    lax.fori_loop(0, n_grp, pull, 0)

    def blank(q, c):
        buf_ref[pl.ds(pl.multiple_of(q * GRP, GRP), GRP), :] = jnp.zeros((GRP, buf_ref.shape[1]), BF16)
        return c

    lax.fori_loop(n_grp, full, blank, 0)
    gates = g_ref[...]
    sel = gates >= 0.0
    tri = (lax.broadcasted_iota(jnp.int32, (BLK, BLK), 1) < lax.broadcasted_iota(jnp.int32, (BLK, BLK), 0)).astype(F32).astype(BF16)
    pos = _dot(tri, jnp.where(sel, 1.0, 0.0).astype(BF16), 1, 0).astype(jnp.int32)
    col_id = lax.broadcasted_iota(jnp.int32, (BLK, n_exp), 1)
    start = jnp.zeros((BLK, n_exp), jnp.int32)
    for e in range(n_exp):
        start = jnp.where(col_id == e, meta_ref[i, e], start)
    slot = jnp.where(sel, pos + start, -1)
    y_ref[...] = jnp.zeros_like(y_ref)
    dx_ref[...] = jnp.zeros_like(dx_ref)
    dg_ref[...] = jnp.zeros_like(dg_ref)

    def done(q, c):
        pltpu.make_async_copy(o_ref.at[pl.ds(0, GRP), :], buf_ref.at[pl.ds(0, GRP), :], sem_ref.at[0]).wait()
        return c

    lax.fori_loop(0, n_grp, done, 0)

    def step(k, c):
        ids = lax.broadcasted_iota(jnp.int32, (BLK, TILE), 1) + k * TILE
        rows = pl.ds(pl.multiple_of(k * TILE, TILE), TILE)
        o = buf_ref[rows, :hidden]
        rg = buf_ref[rows, hidden:]
        prod = _dot(r_ref[...], o, 1, 1)
        hot = jnp.zeros((BLK, TILE), F32)
        gsel = jnp.zeros((BLK, TILE), F32)
        for e in range(n_exp):
            eq = slot[:, e : e + 1] == ids
            hot = jnp.where(eq, 1.0, hot)
            gsel = jnp.where(eq, gates[:, e : e + 1], gsel)
            dg_ref[:, e : e + 1] += jnp.sum(jnp.where(eq, prod, 0.0), axis=1, keepdims=True)
        g_hi = gsel.astype(BF16)
        rest = gsel - g_hi.astype(F32)
        g_mid = rest.astype(BF16)
        g_lo = (rest - g_mid.astype(F32)).astype(BF16)
        y_ref[...] += _dot(g_hi, o, 1, 0) + (_dot(g_mid, o, 1, 0) + _dot(g_lo, o, 1, 0))
        dx_ref[...] += _dot(hot.astype(BF16), rg, 1, 0)
        return c

    lax.fori_loop(0, n_step, step, 0)


def combine(meta, src, rot, gates, r_all, o_rows, n_own):
    n_exp = gates.shape[1]
    width = o_rows.shape[1]
    hidden = width // 2
    n_all = r_all.shape[0] // BLK
    spec = pltpu.PrefetchScalarGridSpec(
        num_scalar_prefetch=3,
        grid=(n_own,),
        in_specs=[
            pl.BlockSpec((BLK, n_exp), lambda i, m, s, r: (lax.rem(r[0] + i, n_all), 0)),
            pl.BlockSpec((BLK, hidden), lambda i, m, s, r: (lax.rem(r[0] + i, n_all), 1)),
            pl.BlockSpec(memory_space=pl.ANY),
        ],
        out_specs=[
            pl.BlockSpec((BLK, hidden), lambda i, m, s, r: (i, 0)),
            pl.BlockSpec((BLK, hidden), lambda i, m, s, r: (i, 0)),
            pl.BlockSpec((BLK, n_exp), lambda i, m, s, r: (i, 0)),
        ],
        scratch_shapes=[pltpu.VMEM((BLK * n_exp, width), BF16), pltpu.SemaphoreType.DMA((1,))],
    )

    def kern(m, s, r, *rest):
        combine_kernel(m, s, *rest, n_exp=n_exp, hidden=hidden)

    return pl.pallas_call(
        kern,
        out_shape=[
            jax.ShapeDtypeStruct((n_own * BLK, hidden), F32),
            jax.ShapeDtypeStruct((n_own * BLK, hidden), F32),
            jax.ShapeDtypeStruct((n_own * BLK, n_exp), F32),
        ],
        grid_spec=spec,
        name="combine",
        cost_estimate=pl.CostEstimate(flops=8_000_000_000, bytes_accessed=20_000_000, transcendentals=0),
    )(meta, src, rot, gates, r_all, o_rows)


def routing_tables(cnt, n_own):
    n_blk, n_exp = cnt.shape
    pad = (cnt + GRP - 1) // GRP * GRP
    before_e = (jnp.arange(n_exp)[:, None] < jnp.arange(n_exp)[None, :]).astype(jnp.int32)
    before_b = (jnp.arange(n_blk)[:, None] < jnp.arange(n_blk)[None, :]).astype(jnp.int32)
    blk_start = jnp.sum(pad[:, :, None] * before_e[None], axis=1)
    blk_end = blk_start + pad
    total = jnp.sum(pad, axis=0)
    base = jnp.sum(total[:, None] * before_e, axis=0)
    in_exp = jnp.sum(pad[:, None, :] * before_b[:, :, None], axis=0)
    own = jnp.sum(pad[:n_own], axis=0)
    own_tiles = (own + TILE - 1) // TILE
    obase = jnp.sum(own_tiles[:, None] * before_e, axis=0) * TILE
    tiles = jnp.maximum((total + TILE - 1) // TILE, 1)
    first = jnp.sum(tiles[:, None] * before_e, axis=0)
    table = jnp.stack([base, total, tiles, own_tiles, first, obase]).astype(jnp.int32)
    q = jnp.arange(BLK * n_exp // GRP, dtype=jnp.int32) * GRP
    inside = (q[None, :, None] >= blk_start[:, None, :]) & (q[None, :, None] < blk_end[:, None, :])
    dst = jnp.sum(jnp.where(inside, (base[None] + in_exp - blk_start)[:, None, :] + q[None, :, None], 0), axis=2)
    src = jnp.sum(jnp.where(inside[:n_own], (obase[None] + in_exp[:n_own] - blk_start[:n_own])[:, None, :] + q[None, :, None], 0), axis=2)
    meta = jnp.concatenate([blk_start, jnp.sum(pad, axis=1, keepdims=True) // GRP], axis=1).astype(jnp.int32)
    return meta, dst.astype(jnp.int32), src.astype(jnp.int32), table


def solution(mesh):
    ep_size = mesh.shape['ep']
    dp_size = mesh.shape['dp']
    n_dev = ep_size * dp_size
    all_axes = ('dp', 'ep')

    def local_step(tokens, w_router, w_gate, w_up, w_down, top_ids, r_proj):
        n_local, hidden = tokens.shape
        n_exp = w_router.shape[1]
        local_exp = w_gate.shape[0]
        dp = lax.axis_index('dp')
        ep = lax.axis_index('ep')
        xr_all = lax.all_gather(jnp.concatenate([tokens, r_proj], axis=1), all_axes, axis=0, tiled=True)
        logits = jnp.dot(tokens, w_router, preferred_element_type=F32)
        hit = top_ids[:, :, None] == jnp.arange(n_exp, dtype=jnp.int32)[None, None, :]
        sel = jnp.any(hit, axis=1)
        peak = jnp.max(jnp.where(sel, logits, -jnp.inf), axis=1, keepdims=True)
        ex = jnp.where(sel, jnp.exp(jnp.where(sel, logits, peak) - peak), 0.0)
        gates = ex / jnp.sum(ex, axis=1, keepdims=True)
        marked = jnp.where(sel, gates, -1.0)
        all_marked = lax.all_gather(marked, all_axes, axis=0, tiled=True)
        mine = lax.dynamic_slice_in_dim(all_marked, ep * local_exp, local_exp, axis=1)
        by_blk = mine.reshape(n_dev, n_local, local_exp)
        order = lax.rem(dp * ep_size + jnp.arange(n_dev, dtype=jnp.int32), n_dev)
        cnt = jnp.sum((by_blk >= 0).astype(jnp.int32), axis=1)[order]
        gates_t = by_blk.transpose(0, 2, 1)[order]
        rot = (dp * ep_size).astype(jnp.int32).reshape(1)
        meta, dst, src, table = routing_tables(cnt, ep_size)
        ud = sort_rows(meta, dst, gates_t, xr_all, rot, n_dev * n_local * local_exp + TILE)
        o_rows, g_gate, g_up, g_down = grouped(table, ud, w_gate, w_up, w_down, ep_size * n_local * local_exp + local_exp * TILE)
        y_part, dx_part, dg_part = combine(meta, src, rot, mine, xr_all, o_rows, ep_size)
        y_sum = lax.psum_scatter(y_part, 'ep', scatter_dimension=0, tiled=True)
        dx_sum = lax.psum_scatter(dx_part, 'ep', scatter_dimension=0, tiled=True)
        dg = lax.all_to_all(dg_part.reshape(ep_size, n_local, local_exp), 'ep', 0, 0, tiled=True)
        dg = dg.transpose(1, 0, 2).reshape(n_local, n_exp)
        dz = (gates * (dg - jnp.sum(gates * dg, axis=1, keepdims=True))).astype(BF16)
        grad_router = lax.psum(_dot(tokens, dz, 0, 0), all_axes)
        y = tokens.astype(F32) + y_sum
        dx = r_proj.astype(F32) + _dot(dz, w_router, 1, 1) + dx_sum
        return y, dx, g_gate, g_up, g_down, grad_router

    tok_spec = P(all_axes, None)
    exp_spec = P('ep', None, None)
    return jax.shard_map(local_step, mesh=mesh, in_specs=(tok_spec, P(), exp_spec, exp_spec, exp_spec, tok_spec, tok_spec), out_specs=(tok_spec, tok_spec, exp_spec, exp_spec, exp_spec, P()), check_vma=False)
```

```python
import functools

import jax
import jax.numpy as jnp
from jax import lax
from jax.experimental import pallas as pl
from jax.experimental.pallas import tpu as pltpu
from jax.sharding import PartitionSpec as P

F32 = jnp.float32
BF16 = jnp.bfloat16
I32 = jnp.int32
GRP = 16
TILE = 256
BLK = 256
PER = TILE // GRP
MESH = pl.DeviceIdType.MESH


def _dot(a, b, ca, cb):
    return lax.dot_general(a, b, (((ca,), (cb,)), ((), ())), preferred_element_type=F32)


def _flip(v, mask):
    for k in range(2):
        if (mask >> k) & 1:
            v = v + (1 << k) * (1 - 2 * ((v // (1 << k)) % 2))
    return v


def _peers(dp, ep, ep_size, n_dev):
    return {r: (_flip(dp, r // ep_size), _flip(ep, r % ep_size)) for r in range(1, n_dev)}


def _greet(peers):
    barrier = pltpu.get_barrier_semaphore()
    for peer in peers.values():
        pl.semaphore_signal(barrier, inc=1, device_id=peer, device_id_type=MESH)
    pl.semaphore_wait(barrier, len(peers))


def gates_kernel(x_ref, wr_ref, ids_ref, out_ref, ssem, rsem, *, n_dev, ep_size):
    dp, ep = lax.axis_index('dp'), lax.axis_index('ep')
    me = dp * ep_size + ep
    peers = _peers(dp, ep, ep_size, n_dev)
    n_exp = wr_ref.shape[1]
    z = _dot(wr_ref[...], x_ref[...], 0, 1)
    eid = lax.broadcasted_iota(I32, z.shape, 0)
    sel = eid == ids_ref[0:1, :]
    for j in range(1, ids_ref.shape[0]):
        sel = jnp.logical_or(sel, eid == ids_ref[j : j + 1, :])
    peak = jnp.max(jnp.where(sel, z, -3.0e38), axis=0, keepdims=True)
    ex = jnp.where(sel, jnp.exp(jnp.where(sel, z - peak, 0.0)), 0.0)
    gates = ex / jnp.sum(ex, axis=0, keepdims=True)
    out_ref[me] = jnp.where(sel, gates, -1.0)
    _greet(peers)
    copies = []
    for r, peer in peers.items():
        copies.append(pltpu.make_async_remote_copy(src_ref=out_ref.at[me], dst_ref=out_ref.at[me], send_sem=ssem.at[r], recv_sem=rsem.at[r], device_id=peer, device_id_type=MESH))
        copies[-1].start()
    for c in copies:
        c.wait()


def share_gates(tokens, w_router, ids_t, n_dev, ep_size):
    n_exp = w_router.shape[1]
    vmem = pl.BlockSpec(memory_space=pltpu.VMEM)
    return pl.pallas_call(
        functools.partial(gates_kernel, n_dev=n_dev, ep_size=ep_size),
        out_shape=jax.ShapeDtypeStruct((n_dev, n_exp, tokens.shape[0]), F32),
        in_specs=[vmem] * 3,
        out_specs=vmem,
        scratch_shapes=[pltpu.SemaphoreType.DMA((n_dev,)), pltpu.SemaphoreType.DMA((n_dev,))],
        compiler_params=pltpu.CompilerParams(collective_id=0, has_side_effects=True),
        cost_estimate=pl.CostEstimate(flops=2_000_000_000, bytes_accessed=2_000_000, transcendentals=0),
        name='share_gates',
    )(tokens, w_router, ids_t)


def router_kernel(dg_ref, g_ref, x_ref, dz_ref, gr_ref, all_ref, part_ref, take_ref, sem_a, sem_b, sem_c, sem_d, sem_e, sem_f, *, n_dev, ep_size):
    dp, ep = lax.axis_index('dp'), lax.axis_index('ep')
    me = dp * ep_size + ep
    peers = _peers(dp, ep, ep_size, n_dev)
    local = dg_ref.shape[1]
    all_ref[ep] = dg_ref[0]
    _greet(peers)
    copies = []
    for r in range(1, ep_size):
        copies.append(pltpu.make_async_remote_copy(src_ref=dg_ref.at[r], dst_ref=all_ref.at[ep], send_sem=sem_a.at[r], recv_sem=sem_b.at[r], device_id=peers[r], device_id_type=MESH))
        copies[-1].start()
    for c in copies:
        c.wait()
    g = jnp.maximum(g_ref[me], 0.0)
    dg = jnp.concatenate([all_ref[k] for k in range(ep_size)], axis=0)
    dz = (g * (dg - jnp.sum(g * dg, axis=0, keepdims=True))).astype(BF16)
    dz_ref[...] = dz
    part = _dot(dz, x_ref[...], 1, 0)
    rows = part.shape[0] // n_dev
    for k in range(n_dev):
        part_ref[k] = part[k * rows : (k + 1) * rows, :]
    take_ref[me] = part_ref[me]
    copies = []
    for r, peer in peers.items():
        pid = peer[0] * ep_size + peer[1]
        copies.append(pltpu.make_async_remote_copy(src_ref=part_ref.at[pid], dst_ref=take_ref.at[me], send_sem=sem_c.at[r], recv_sem=sem_d.at[r], device_id=peer, device_id_type=MESH))
        copies[-1].start()
    for c in copies:
        c.wait()
    total = take_ref[0]
    for k in range(1, n_dev):
        total = total + take_ref[k]
    gr_ref[me] = total
    copies = []
    for r, peer in peers.items():
        copies.append(pltpu.make_async_remote_copy(src_ref=gr_ref.at[me], dst_ref=gr_ref.at[me], send_sem=sem_e.at[r], recv_sem=sem_f.at[r], device_id=peer, device_id_type=MESH))
        copies[-1].start()
    for c in copies:
        c.wait()


def router_backward(dg, gates, tokens, n_dev, ep_size):
    n_exp = gates.shape[1]
    n_tok, hidden = tokens.shape
    vmem = pl.BlockSpec(memory_space=pltpu.VMEM)
    rows = n_exp // n_dev
    dma = pltpu.SemaphoreType.DMA((n_dev,))
    return pl.pallas_call(
        functools.partial(router_kernel, n_dev=n_dev, ep_size=ep_size),
        out_shape=[jax.ShapeDtypeStruct((n_exp, n_tok), BF16), jax.ShapeDtypeStruct((n_dev, rows, hidden), F32)],
        in_specs=[vmem] * 3,
        out_specs=[vmem] * 2,
        scratch_shapes=[
            pltpu.VMEM((ep_size, n_exp // ep_size, n_tok), F32),
            pltpu.VMEM((n_dev, rows, hidden), F32),
            pltpu.VMEM((n_dev, rows, hidden), F32),
            *([dma] * 6),
        ],
        compiler_params=pltpu.CompilerParams(collective_id=1, has_side_effects=True),
        cost_estimate=pl.CostEstimate(flops=2_000_000_000, bytes_accessed=2_000_000, transcendentals=0),
        name='router_backward',
    )(dg, gates, tokens)


def _slots(meta_ref, i, gates_t, slot_ref):
    n_exp = gates_t.shape[0]
    sel = gates_t >= 0.0
    tri = (lax.broadcasted_iota(I32, (BLK, BLK), 0) < lax.broadcasted_iota(I32, (BLK, BLK), 1)).astype(F32).astype(BF16)
    pos = _dot(jnp.where(sel, 1.0, 0.0).astype(BF16), tri, 1, 0).astype(I32)
    row_id = lax.broadcasted_iota(I32, (n_exp, BLK), 0)
    start = jnp.zeros((n_exp, BLK), I32)
    for e in range(n_exp):
        start = jnp.where(row_id == e, meta_ref[i, e], start)
    slot_ref[...] = jnp.where(sel, pos + start, -1)


def sort_kernel(meta_ref, dst_ref, zero_ref, me_ref, gt_ref, *rest, n_exp, n_blk, skip):
    srcs = rest[:n_blk]
    out_ref, slot_ref, x_ref, buf_ref, zbuf_ref, pend_ref, xsem, sem_ref, zsem = rest[n_blk:]
    i = pl.program_id(0)
    hidden = x_ref.shape[2] // 2
    par = lax.rem(i, 2)

    def load(k, s):
        return pltpu.make_async_copy(srcs[k], x_ref.at[s], xsem.at[s])

    def zeros(q):
        return pltpu.make_async_copy(zbuf_ref, out_ref.at[pl.ds(pl.multiple_of(q * GRP, GRP), GRP), :], zsem.at[0])

    @pl.when(i == 0)
    def _():
        load(0, 0).start()
        pend_ref[0] = 0
        pend_ref[1] = 0
        pend_ref[2] = 0
        zbuf_ref[...] = jnp.zeros_like(zbuf_ref)
        for e in range(n_exp):
            lax.fori_loop(0, zero_ref[1, e], lambda q, c: (zeros(zero_ref[0, e] + q).start(), c)[1], 0)

    for k in range(n_blk - 1):

        @pl.when(i == k)
        def _():
            load(k + 1, (k + 1) % 2).start()

    n_grp = meta_ref[skip + i, n_exp]
    n_step = (n_grp + PER - 1) // PER
    _slots(meta_ref, skip + i, gt_ref[0], slot_ref)
    load(0, par).wait()

    def drain(s):
        cnt = pend_ref[s]

        @pl.when(cnt == PER)
        def _():
            pltpu.make_async_copy(buf_ref.at[0], out_ref.at[pl.ds(0, TILE), :], sem_ref.at[s]).wait()

        @pl.when(cnt < PER)
        def _():
            def one(_, c):
                pltpu.make_async_copy(buf_ref.at[0, pl.ds(0, GRP), :], out_ref.at[pl.ds(0, GRP), :], sem_ref.at[s]).wait()
                return c

            lax.fori_loop(0, cnt, one, 0)

    def step(k, c):
        s = lax.rem(pend_ref[2], 2)
        pend_ref[2] = pend_ref[2] + 1
        ids = lax.broadcasted_iota(I32, (TILE, BLK), 0) + k * TILE
        hot = jnp.zeros((TILE, BLK), F32)
        gsel = jnp.zeros((TILE, BLK), F32)
        for e in range(n_exp):
            eq = slot_ref[e : e + 1, :] == ids
            hot = jnp.where(eq, 1.0, hot)
            gsel = jnp.where(eq, gt_ref[0, e : e + 1, :], gsel)
        hot = hot.astype(BF16)
        gcol = jnp.sum(gsel, axis=1, keepdims=True)
        drain(s)
        buf_ref[s, :, :hidden] = _dot(hot, x_ref[par, :, :hidden], 1, 0).astype(BF16)
        buf_ref[s, :, hidden:] = (gcol * _dot(hot, x_ref[par, :, hidden:], 1, 0)).astype(BF16)
        cnt = jnp.minimum(n_grp - k * PER, PER)
        pend_ref[s] = cnt

        def send(q, c):
            dst = pl.multiple_of(dst_ref[skip + i, k * PER + q], GRP)
            pltpu.make_async_copy(buf_ref.at[s, pl.ds(pl.multiple_of(q * GRP, GRP), GRP), :], out_ref.at[pl.ds(dst, GRP), :], sem_ref.at[s]).start()
            return c

        lax.fori_loop(0, cnt, send, 0)
        return c

    lax.fori_loop(0, n_step, step, 0)

    @pl.when(i == n_blk - 1)
    def _():
        drain(0)
        drain(1)
        for e in range(n_exp):
            lax.fori_loop(0, zero_ref[1, e], lambda q, c: (zeros(0).wait(), c)[1], 0)


def sort_rows(meta, dst, zero, me, gates_t, blocks, skip, rows, ep, name):
    n_exp = meta.shape[1] - 1
    n_blk = len(blocks)
    width = blocks[0].shape[1]
    spec = pltpu.PrefetchScalarGridSpec(
        num_scalar_prefetch=4,
        grid=(n_blk,),
        in_specs=[pl.BlockSpec((1, n_exp, BLK), lambda i, m, d, z, r: (r[0] ^ (skip + i), r[1], 0))] + [pl.BlockSpec(memory_space=pl.ANY)] * n_blk,
        out_specs=pl.BlockSpec(memory_space=pl.ANY),
        scratch_shapes=[
            pltpu.VMEM((n_exp, BLK), I32),
            pltpu.VMEM((2, BLK, width), BF16),
            pltpu.VMEM((2, TILE, width), BF16),
            pltpu.VMEM((GRP, width), BF16),
            pltpu.SMEM((3,), I32),
            pltpu.SemaphoreType.DMA((2,)),
            pltpu.SemaphoreType.DMA((2,)),
            pltpu.SemaphoreType.DMA((1,)),
        ],
    )
    return pl.pallas_call(
        functools.partial(sort_kernel, n_exp=n_exp, n_blk=n_blk, skip=skip),
        out_shape=jax.ShapeDtypeStruct((rows, width), BF16),
        grid_spec=spec,
        name=name,
        cost_estimate=pl.CostEstimate(flops=1_500_000_000 * n_blk, bytes_accessed=3_000_000 * n_blk, transcendentals=0),
    )(meta, dst, zero, me, gates_t, *blocks)


def own_kernel(t_ref, ud_ref, w1_ref, w3_ref, w2_ref, o_ref, sv_ref, in_ref, ob_ref, sb_ref, isem, osem, ssem, *, n_exp, hidden, inner):
    e = pl.program_id(0)
    first, n_tile = t_ref[0, e], t_ref[1, e]
    total = t_ref[0, n_exp - 1] + t_ref[1, n_exp - 1]

    def rows(g):
        return pl.ds(pl.multiple_of(g * TILE, TILE), TILE)

    def fetch(g, s):
        return pltpu.make_async_copy(ud_ref.at[rows(g), :], in_ref.at[s], isem.at[s])

    def put(g, s):
        return pltpu.make_async_copy(ob_ref.at[s], o_ref.at[rows(g), :], osem.at[s])

    def save(g, s):
        return pltpu.make_async_copy(sb_ref.at[s], sv_ref.at[rows(g), :], ssem.at[s])

    @pl.when(e == 0)
    def _():
        fetch(0, 0).start()

    def tile(k, c):
        g = first + k
        s = lax.rem(g, 2)
        fetch(g, s).wait()

        @pl.when(g + 1 < total)
        def _():
            fetch(g + 1, 1 - s).start()

        @pl.when(g >= 2)
        def _():
            put(0, s).wait()
            save(0, s).wait()

        u = in_ref[s, :, :hidden]
        d = in_ref[s, :, hidden:]
        h1 = _dot(u, w1_ref[0], 1, 0)
        h3 = _dot(u, w3_ref[0], 1, 0)
        da = _dot(d, w2_ref[0], 1, 1)
        sig = jax.nn.sigmoid(h1)
        silu = h1 * sig
        act = (silu * h3).astype(BF16)
        dh1 = (da * h3 * sig * (1.0 + h1 * (1.0 - sig))).astype(BF16)
        dh3 = (da * silu).astype(BF16)
        sb_ref[s, :, :inner] = act
        sb_ref[s, :, inner : 2 * inner] = dh1
        sb_ref[s, :, 2 * inner :] = dh3
        ob_ref[s, :, :hidden] = _dot(act, w2_ref[0], 1, 0).astype(BF16)
        ob_ref[s, :, hidden:] = (_dot(dh1, w1_ref[0], 1, 1) + _dot(dh3, w3_ref[0], 1, 1)).astype(BF16)
        put(g, s).start()
        save(g, s).start()
        return c

    lax.fori_loop(0, n_tile, tile, 0)

    @pl.when(e == n_exp - 1)
    def _():
        for s in range(2):
            put(0, s).wait()
            save(0, s).wait()


def own_rows(table, ud, w1, w3, w2):
    n_exp, hidden, inner = w1.shape
    n_row, width = ud.shape
    wspec = lambda a, b: pl.BlockSpec((1, a, b), lambda e, t: (e, 0, 0))
    hbm = pl.BlockSpec(memory_space=pl.ANY)
    spec = pltpu.PrefetchScalarGridSpec(
        num_scalar_prefetch=1,
        grid=(n_exp,),
        in_specs=[hbm, wspec(hidden, inner), wspec(hidden, inner), wspec(inner, hidden)],
        out_specs=[hbm, hbm],
        scratch_shapes=[
            pltpu.VMEM((2, TILE, width), BF16),
            pltpu.VMEM((2, TILE, width), BF16),
            pltpu.VMEM((2, TILE, 3 * inner), BF16),
            pltpu.SemaphoreType.DMA((2,)),
            pltpu.SemaphoreType.DMA((2,)),
            pltpu.SemaphoreType.DMA((2,)),
        ],
    )
    return pl.pallas_call(
        functools.partial(own_kernel, n_exp=n_exp, hidden=hidden, inner=inner),
        out_shape=[jax.ShapeDtypeStruct((n_row, width), BF16), jax.ShapeDtypeStruct((n_row, 3 * inner), BF16)],
        grid_spec=spec,
        name='own_rows',
        cost_estimate=pl.CostEstimate(flops=30_000_000_000, bytes_accessed=60_000_000, transcendentals=2_000_000),
    )(table, ud, w1, w3, w2)


def grads_kernel(ta_ref, tb_ref, uo_ref, sv_ref, ud_ref, w1_ref, w3_ref, w2_ref, g1_ref, g3_ref, g2_ref, oin_ref, sin_ref, in_ref, osem, ssem, isem, *, n_exp, hidden, inner):
    e = pl.program_id(0)

    def rows(g):
        return pl.ds(pl.multiple_of(g * TILE, TILE), TILE)

    def fetch(g, s):
        return pltpu.make_async_copy(ud_ref.at[rows(g), :], in_ref.at[s], isem.at[s])

    def own(g, s):
        return pltpu.make_async_copy(uo_ref.at[rows(g), :], oin_ref.at[s], osem.at[s])

    def saved(g, s):
        return pltpu.make_async_copy(sv_ref.at[rows(g), :], sin_ref.at[s], ssem.at[s])

    @pl.when(e == 0)
    def _():
        own(0, 0).start()
        saved(0, 0).start()
        fetch(0, 0).start()

    g1_ref[...] = jnp.zeros_like(g1_ref)
    g3_ref[...] = jnp.zeros_like(g3_ref)
    g2_ref[...] = jnp.zeros_like(g2_ref)
    o_total = ta_ref[0, n_exp - 1] + ta_ref[1, n_exp - 1]
    total = tb_ref[0, n_exp - 1] + tb_ref[1, n_exp - 1]

    def own_tile(k, c):
        g = ta_ref[0, e] + k
        s = lax.rem(g, 2)
        own(g, s).wait()
        saved(g, s).wait()

        @pl.when(g + 1 < o_total)
        def _():
            own(g + 1, 1 - s).start()
            saved(g + 1, 1 - s).start()

        u = oin_ref[s, :, :hidden]
        d = oin_ref[s, :, hidden:]
        g1_ref[0] += _dot(u, sin_ref[s, :, inner : 2 * inner], 0, 0)
        g3_ref[0] += _dot(u, sin_ref[s, :, 2 * inner :], 0, 0)
        g2_ref[0] += _dot(sin_ref[s, :, :inner], d, 0, 0)
        return c

    lax.fori_loop(0, ta_ref[1, e], own_tile, 0)

    def tile(k, c):
        g = tb_ref[0, e] + k
        s = lax.rem(g, 2)
        fetch(g, s).wait()

        @pl.when(g + 1 < total)
        def _():
            fetch(g + 1, 1 - s).start()

        u = in_ref[s, :, :hidden]
        d = in_ref[s, :, hidden:]
        h1 = _dot(u, w1_ref[0], 1, 0)
        h3 = _dot(u, w3_ref[0], 1, 0)
        da = _dot(d, w2_ref[0], 1, 1)
        sig = jax.nn.sigmoid(h1)
        silu = h1 * sig
        act = (silu * h3).astype(BF16)
        dh1 = (da * h3 * sig * (1.0 + h1 * (1.0 - sig))).astype(BF16)
        dh3 = (da * silu).astype(BF16)
        g1_ref[0] += _dot(u, dh1, 0, 0)
        g3_ref[0] += _dot(u, dh3, 0, 0)
        g2_ref[0] += _dot(act, d, 0, 0)
        return c

    lax.fori_loop(0, tb_ref[1, e], tile, 0)


def weight_grads(ta, tb, uo, sv, ud, w1, w3, w2):
    n_exp, hidden, inner = w1.shape
    width = ud.shape[1]
    wspec = lambda a, b: pl.BlockSpec((1, a, b), lambda e, t, s: (e, 0, 0))
    hbm = pl.BlockSpec(memory_space=pl.ANY)
    spec = pltpu.PrefetchScalarGridSpec(
        num_scalar_prefetch=2,
        grid=(n_exp,),
        in_specs=[hbm, hbm, hbm, wspec(hidden, inner), wspec(hidden, inner), wspec(inner, hidden)],
        out_specs=[wspec(hidden, inner), wspec(hidden, inner), wspec(inner, hidden)],
        scratch_shapes=[
            pltpu.VMEM((2, TILE, width), BF16),
            pltpu.VMEM((2, TILE, 3 * inner), BF16),
            pltpu.VMEM((2, TILE, width), BF16),
            pltpu.SemaphoreType.DMA((2,)),
            pltpu.SemaphoreType.DMA((2,)),
            pltpu.SemaphoreType.DMA((2,)),
        ],
    )
    return pl.pallas_call(
        functools.partial(grads_kernel, n_exp=n_exp, hidden=hidden, inner=inner),
        out_shape=[jax.ShapeDtypeStruct(w.shape, F32) for w in (w1, w3, w2)],
        grid_spec=spec,
        name='weight_grads',
        cost_estimate=pl.CostEstimate(flops=90_000_000_000, bytes_accessed=150_000_000, transcendentals=4_000_000),
    )(ta, tb, uo, sv, ud, w1, w3, w2)


def combine_kernel(meta_ref, src_ref, me_ref, g_ref, r_ref_a, r_ref_b, o_ref, p_ref, dg_ref, slot_ref, buf_ref, sem_ref, *, n_exp, hidden, which):
    i = pl.program_id(0)
    par = lax.rem(i, 2)

    def rel(k):
        return which[0] + k * (which[1] - which[0])

    def pull(k, s):
        def one(q, c):
            src = pl.multiple_of(src_ref[rel(k), q], GRP)
            pltpu.make_async_copy(o_ref.at[pl.ds(src, GRP), :], buf_ref.at[s, pl.ds(pl.multiple_of(q * GRP, GRP), GRP), :], sem_ref.at[s]).start()
            return c

        lax.fori_loop(0, meta_ref[rel(k), n_exp], one, 0)

    @pl.when(i == 0)
    def _():
        pull(0, 0)
        pull(1, 1)

    n_grp = meta_ref[rel(i), n_exp]
    n_step = (n_grp + PER - 1) // PER

    def blank(q, c):
        buf_ref[par, pl.ds(pl.multiple_of(q * GRP, GRP), GRP), :] = jnp.zeros((GRP, buf_ref.shape[2]), BF16)
        return c

    lax.fori_loop(n_grp, n_step * PER, blank, 0)
    _slots(meta_ref, rel(i), g_ref[0], slot_ref)
    p_ref[...] = jnp.zeros_like(p_ref)
    dg_ref[...] = jnp.zeros_like(dg_ref)

    def whole(q, c):
        pltpu.make_async_copy(o_ref.at[pl.ds(0, TILE), :], buf_ref.at[0, pl.ds(0, TILE), :], sem_ref.at[par]).wait()
        return c

    def single(q, c):
        pltpu.make_async_copy(o_ref.at[pl.ds(0, GRP), :], buf_ref.at[0, pl.ds(0, GRP), :], sem_ref.at[par]).wait()
        return c

    lax.fori_loop(0, n_grp // PER, whole, 0)
    lax.fori_loop(0, lax.rem(n_grp, PER), single, 0)
    r_blk = jnp.where(i == 0, r_ref_a[...], r_ref_b[...])

    def step(k, c):
        ids = lax.broadcasted_iota(I32, (TILE, BLK), 0) + k * TILE
        rows = pl.ds(pl.multiple_of(k * TILE, TILE), TILE)
        o = buf_ref[par, rows, :hidden]
        rg = buf_ref[par, rows, hidden:]
        prod = _dot(o, r_blk, 1, 1)
        hot = jnp.zeros((TILE, BLK), F32)
        gsel = jnp.zeros((TILE, BLK), F32)
        for e in range(n_exp):
            eq = slot_ref[e : e + 1, :] == ids
            hot = jnp.where(eq, 1.0, hot)
            gsel = jnp.where(eq, g_ref[0, e : e + 1, :], gsel)
            dg_ref[0, e : e + 1, :] += jnp.sum(jnp.where(eq, prod, 0.0), axis=0, keepdims=True)
        g_hi = gsel.astype(BF16)
        rest = gsel - g_hi.astype(F32)
        g_mid = rest.astype(BF16)
        g_lo = (rest - g_mid.astype(F32)).astype(BF16)
        p_ref[:, :hidden] += _dot(g_hi, o, 0, 0) + (_dot(g_mid, o, 0, 0) + _dot(g_lo, o, 0, 0))
        p_ref[:, hidden:] += _dot(hot.astype(BF16), rg, 0, 0)
        return c

    lax.fori_loop(0, n_step, step, 0)


def combine(meta, src, me, gates, blocks, o_rows, which):
    n_exp = meta.shape[1] - 1
    width = o_rows.shape[1]
    hidden = width // 2
    half = pl.BlockSpec((BLK, hidden), lambda i, m, s, r: (0, 1))
    spec = pltpu.PrefetchScalarGridSpec(
        num_scalar_prefetch=3,
        grid=(2,),
        in_specs=[
            pl.BlockSpec((1, n_exp, BLK), lambda i, m, s, r: (r[0] ^ (which[0] + i * (which[1] - which[0])), r[1], 0)),
            half,
            half,
            pl.BlockSpec(memory_space=pl.ANY),
        ],
        out_specs=[
            pl.BlockSpec((BLK, width), lambda i, m, s, r: (i, 0)),
            pl.BlockSpec((1, n_exp, BLK), lambda i, m, s, r: (i, 0, 0)),
        ],
        scratch_shapes=[pltpu.VMEM((n_exp, BLK), I32), pltpu.VMEM((2, BLK * n_exp, width), BF16), pltpu.SemaphoreType.DMA((2,))],
    )
    return pl.pallas_call(
        functools.partial(combine_kernel, n_exp=n_exp, hidden=hidden, which=which),
        out_shape=[jax.ShapeDtypeStruct((2 * BLK, width), F32), jax.ShapeDtypeStruct((2, n_exp, BLK), F32)],
        grid_spec=spec,
        name='combine',
        cost_estimate=pl.CostEstimate(flops=8_000_000_000, bytes_accessed=20_000_000, transcendentals=0),
    )(meta, src, me, gates, blocks[which[0]], blocks[which[1]], o_rows)


def routing_tables(cnt, n_own):
    n_blk, n_exp = cnt.shape
    pad = (cnt + GRP - 1) // GRP * GRP
    before_e = (jnp.arange(n_exp)[:, None] < jnp.arange(n_exp)[None, :]).astype(I32)
    blk = jnp.arange(n_blk)
    same = (blk[:, None] < n_own) == (blk[None, :] < n_own)
    before_b = ((blk[:, None] < blk[None, :]) & same).astype(I32)
    blk_start = jnp.sum(pad[:, :, None] * before_e[None], axis=1)
    blk_end = blk_start + pad
    in_exp = jnp.sum(pad[:, None, :] * before_b[:, :, None], axis=0)

    def part(p):
        total = jnp.sum(p, axis=0)
        tiles = jnp.maximum((total + TILE - 1) // TILE, 1)
        first = jnp.sum(tiles[:, None] * before_e, axis=0)
        zero = jnp.stack([(first * TILE + total) // GRP, (tiles * TILE - total) // GRP])
        return jnp.stack([first, tiles]).astype(I32), zero.astype(I32), first * TILE

    ta, za, base_a = part(pad[:n_own])
    tb, zb, base_b = part(pad[n_own:])
    base = jnp.where(blk[:, None] < n_own, base_a[None], base_b[None])
    q = jnp.arange(BLK * n_exp // GRP, dtype=I32) * GRP
    inside = (q[None, :, None] >= blk_start[:, None, :]) & (q[None, :, None] < blk_end[:, None, :])
    dst = jnp.sum(jnp.where(inside, (base + in_exp - blk_start)[:, None, :] + q[None, :, None], 0), axis=2)
    meta = jnp.concatenate([blk_start, jnp.sum(pad, axis=1, keepdims=True) // GRP], axis=1).astype(I32)
    return meta, dst.astype(I32), ta, za, tb, zb


def solution(mesh):
    ep_size = mesh.shape['ep']
    dp_size = mesh.shape['dp']
    n_dev = ep_size * dp_size
    all_axes = ('dp', 'ep')

    def swap(v, mask):
        return lax.ppermute(v, all_axes, [(d, d ^ mask) for d in range(n_dev)])

    def local_step(tokens, w_router, w_gate, w_up, w_down, top_ids, r_proj):
        n_local, hidden = tokens.shape
        n_exp = w_router.shape[1]
        local_exp = w_gate.shape[0]
        dp = lax.axis_index('dp')
        ep = lax.axis_index('ep')
        me = jnp.stack([dp * ep_size + ep, ep]).astype(I32)
        xr = jnp.concatenate([tokens, r_proj], axis=1)
        blk = {0: xr}
        blk[2] = swap(xr, 2)
        blk[4] = swap(xr, 4)
        blk[8] = swap(xr, 8)
        blk[1] = swap(xr, 1)
        blk[3] = swap(blk[2], 1)
        gates = share_gates(tokens, w_router, top_ids.T, n_dev, ep_size)
        mine = lax.dynamic_slice_in_dim(gates, ep * local_exp, local_exp, axis=1)
        cnt_all = jnp.sum((mine >= 0).astype(I32), axis=2)
        order = me[0] ^ jnp.arange(n_dev, dtype=I32)
        pick = (order[:, None] == jnp.arange(n_dev, dtype=I32)[None, :]).astype(I32)
        cnt = jnp.sum(pick[:, :, None] * cnt_all[None], axis=1)
        meta, dst, ta, za, tb, zb = routing_tables(cnt, ep_size)
        blk[6] = swap(blk[4], 2)
        blk[12] = swap(blk[8], 4)
        blk[10] = swap(blk[2], 8)
        blk[5] = swap(blk[4], 1)
        blk[9] = swap(blk[8], 1)
        own_n = ep_size * n_local * local_exp + local_exp * TILE
        oth_n = (n_dev - ep_size) * n_local * local_exp + local_exp * TILE
        uo = sort_rows(meta, dst, za, me, gates, [blk[k] for k in range(4)], 0, own_n, ep, 'sort_own')
        o_rows, sv = own_rows(ta, uo, w_gate, w_up, w_down)
        p_send, dg_b = combine(meta, dst, me, gates, blk, o_rows, (1, 3))
        p_sib = swap(p_send, 1)
        p_keep, dg_a = combine(meta, dst, me, gates, blk, o_rows, (0, 2))
        cut = (96, 80)
        c0, c1 = cut[0], cut[0] + cut[1]
        far = [swap(blk[12][:c0], 2), swap(blk[10][c0:c1], 4), swap(blk[6][c1:], 8)]
        blk[14] = jnp.concatenate(far, axis=0)
        for k in (6, 10, 12, 14):
            blk[k + 1] = swap(blk[k], 1)
        p_mine = p_keep[:BLK] + p_sib[:BLK]
        p_far = swap(p_keep[BLK:] + p_sib[BLK:], 2)
        dg = jnp.stack([dg_a[0], dg_b[0], dg_a[1], dg_b[1]])
        dz_t, grad_router_t = router_backward(dg, gates, tokens, n_dev, ep_size)
        ud = sort_rows(meta, dst, zb, me, gates, [blk[k] for k in range(4, 16)], 4, oth_n, ep, 'sort_other')
        g_gate, g_up, g_down = weight_grads(ta, tb, uo, sv, ud, w_gate, w_up, w_down)
        grad_router = grad_router_t.reshape(n_exp, hidden).T
        y = tokens.astype(F32) + (p_mine[:, :hidden] + p_far[:, :hidden])
        dx = r_proj.astype(F32) + _dot(dz_t, w_router, 0, 1) + (p_mine[:, hidden:] + p_far[:, hidden:])
        return y, dx, g_gate, g_up, g_down, grad_router

    tok_spec = P(all_axes, None)
    exp_spec = P('ep', None, None)
    return jax.shard_map(local_step, mesh=mesh, in_specs=(tok_spec, P(), exp_spec, exp_spec, exp_spec, tok_spec, tok_spec), out_specs=(tok_spec, tok_spec, exp_spec, exp_spec, exp_spec, P()), check_vma=False)
```

```python
import functools

import jax
import jax.numpy as jnp
from jax import lax
from jax.experimental import pallas as pl
from jax.experimental.pallas import tpu as pltpu
from jax.sharding import PartitionSpec as P


F32 = jnp.float32
BF16 = jnp.bfloat16
I32 = jnp.int32
GRP = 16
UNIT = 128
MOST = 4
STEP = 256
BLK = 256
PER = STEP // GRP
MESH = pl.DeviceIdType.MESH


def _dot(a, b, ca, cb):
    return lax.dot_general(a, b, (((ca,), (cb,)), ((), ())), preferred_element_type=F32)


def _flip(v, mask):
    for k in range(2):
        if (mask >> k) & 1:
            v = v + (1 << k) * (1 - 2 * ((v // (1 << k)) % 2))
    return v


def _peers(dp, ep, ep_size, n_dev):
    return {r: (_flip(dp, r // ep_size), _flip(ep, r % ep_size)) for r in range(1, n_dev)}


def _greet(peers):
    barrier = pltpu.get_barrier_semaphore()
    for peer in peers.values():
        pl.semaphore_signal(barrier, inc=1, device_id=peer, device_id_type=MESH)
    pl.semaphore_wait(barrier, len(peers))


def first_kernel(x_ref, wr_ref, ids_ref, xr_ref, own_ref, out_ref, b1, b2, b4, b8, b3, b5, b9, ssem, rsem, bsend, brecv, fsend, frecv, *, n_dev, ep_size):
    dp, ep = lax.axis_index('dp'), lax.axis_index('ep')
    peers = _peers(dp, ep, ep_size, n_dev)
    local = out_ref.shape[1]
    _greet(peers)

    def copy(src, dst, s, r, k, mask):
        return pltpu.make_async_remote_copy(src_ref=src, dst_ref=dst, send_sem=s.at[k], recv_sem=r.at[k], device_id=peers[mask], device_id_type=MESH)

    half = xr_ref.shape[0] // 2
    part = [pl.ds(0, half), pl.ds(half, half)]
    direct = []
    for h in range(2):
        for k, (dst, mask) in enumerate(((b2, 2), (b4, 4), (b8, 8), (b1, 1))):
            direct.append(copy(xr_ref.at[part[h], :], dst.at[part[h], :], bsend, brecv, 4 * h + k, mask))
            direct[-1].start()
    z = _dot(wr_ref[...], x_ref[...], 0, 1)
    eid = lax.broadcasted_iota(I32, z.shape, 0)
    sel = eid == ids_ref[0:1, :]
    for j in range(1, ids_ref.shape[0]):
        sel = jnp.logical_or(sel, eid == ids_ref[j : j + 1, :])
    peak = jnp.max(jnp.where(sel, z, -3.0e38), axis=0, keepdims=True)
    ex = jnp.where(sel, jnp.exp(jnp.where(sel, z - peak, 0.0)), 0.0)
    gates = ex / jnp.sum(ex, axis=0, keepdims=True)
    marked = jnp.where(sel, gates, -1.0)
    for k in range(ep_size):
        own_ref[k] = marked[k * local : (k + 1) * local, :]
    out_ref[0] = own_ref[ep]
    direct[3].wait_recv()
    small = [copy(own_ref.at[peer[1]], out_ref.at[r], ssem, rsem, r, r) for r, peer in peers.items()]
    for c in small:
        c.start()
    passed = []
    for h in range(2):
        for k, (src, dst) in enumerate(((b2, b3), (b4, b5), (b8, b9))):
            direct[4 * h + k].wait_recv()
            passed.append(copy(src.at[part[h], :], dst.at[part[h], :], fsend, frecv, 3 * h + k, 1))
            passed[-1].start()
    direct[7].wait_recv()
    for c in direct:
        c.wait_send()
    for c in passed + small:
        c.wait()


def first_stage(tokens, w_router, ids_t, xr, n_dev, ep_size):
    local = w_router.shape[1] // ep_size
    n_tok = tokens.shape[0]
    vmem = pl.BlockSpec(memory_space=pltpu.VMEM)
    hbm = pl.BlockSpec(memory_space=pl.ANY)
    dma = pltpu.SemaphoreType.DMA
    return pl.pallas_call(
        functools.partial(first_kernel, n_dev=n_dev, ep_size=ep_size),
        out_shape=[jax.ShapeDtypeStruct((ep_size, local, n_tok), F32), jax.ShapeDtypeStruct((n_dev, local, n_tok), F32)] + [jax.ShapeDtypeStruct(xr.shape, BF16)] * 7,
        in_specs=[vmem] * 3 + [hbm],
        out_specs=[vmem] * 2 + [hbm] * 7,
        scratch_shapes=[dma((n_dev,)), dma((n_dev,)), dma((8,)), dma((8,)), dma((6,)), dma((6,))],
        compiler_params=pltpu.CompilerParams(collective_id=0, has_side_effects=True),
        cost_estimate=pl.CostEstimate(flops=20_000_000_000, bytes_accessed=20_000_000, transcendentals=0),
        name='first_stage',
    )(tokens, w_router, ids_t, xr)


def last_kernel(b6, b10, b12, b7, b11, b13, b14, b15, ssem, rsem, *, n_dev, ep_size):
    dp, ep = lax.axis_index('dp'), lax.axis_index('ep')
    every = _peers(dp, ep, ep_size, n_dev)
    peers = {m: every[m] for m in (1, 2, 4, 8)}
    _greet(peers)

    def copy(src, dst, k, mask):
        return pltpu.make_async_remote_copy(src_ref=src, dst_ref=dst, send_sem=ssem.at[k], recv_sem=rsem.at[k], device_id=peers[mask], device_id_type=MESH)

    n_row = b6.shape[0]
    c0 = n_row // 3 // GRP * GRP + GRP
    c1 = (c0 + n_row) // 2 // GRP * GRP
    far = []
    for k, (src, mask, lo, hi) in enumerate(((b12, 2, 0, c0), (b10, 4, c0, c1), (b6, 8, c1, n_row))):
        far.append(copy(src.at[pl.ds(lo, hi - lo), :], b14.at[pl.ds(lo, hi - lo), :], k, mask))
        far[-1].start()
    near = [copy(src, dst, 3 + k, 1) for k, (src, dst) in enumerate(((b6, b7), (b10, b11), (b12, b13)))]
    for c in near:
        c.start()
    for c in far:
        c.wait_recv()
    end = copy(b14, b15, 6, 1)
    end.start()
    for c in far:
        c.wait_send()
    for c in near:
        c.wait()
    end.wait()


def last_stage(b6, b10, b12, n_dev, ep_size):
    hbm = pl.BlockSpec(memory_space=pl.ANY)
    return pl.pallas_call(
        functools.partial(last_kernel, n_dev=n_dev, ep_size=ep_size),
        out_shape=[jax.ShapeDtypeStruct(b6.shape, BF16)] * 5,
        in_specs=[hbm] * 3,
        out_specs=[hbm] * 5,
        scratch_shapes=[pltpu.SemaphoreType.DMA((7,)), pltpu.SemaphoreType.DMA((7,))],
        compiler_params=pltpu.CompilerParams(collective_id=2, has_side_effects=True),
        cost_estimate=pl.CostEstimate(flops=10_000_000_000, bytes_accessed=10_000_000, transcendentals=0),
        name='last_stage',
    )(b6, b10, b12)


def router_kernel(dg_ref, g_ref, x_ref, dz_ref, gr_ref, all_ref, part_ref, take_ref, sem_a, sem_b, sem_c, sem_d, sem_e, sem_f, *, n_dev, ep_size):
    dp, ep = lax.axis_index('dp'), lax.axis_index('ep')
    me = dp * ep_size + ep
    peers = _peers(dp, ep, ep_size, n_dev)
    all_ref[ep] = dg_ref[0]
    _greet(peers)
    copies = []
    for r in range(1, ep_size):
        copies.append(pltpu.make_async_remote_copy(src_ref=dg_ref.at[r], dst_ref=all_ref.at[ep], send_sem=sem_a.at[r], recv_sem=sem_b.at[r], device_id=peers[r], device_id_type=MESH))
        copies[-1].start()
    for c in copies:
        c.wait()
    g = jnp.maximum(jnp.concatenate([g_ref[k] for k in range(ep_size)], axis=0), 0.0)
    dg = jnp.concatenate([all_ref[k] for k in range(ep_size)], axis=0)
    dz = (g * (dg - jnp.sum(g * dg, axis=0, keepdims=True))).astype(BF16)
    dz_ref[...] = dz
    part = _dot(dz, x_ref[...], 1, 0)
    rows = part.shape[0] // n_dev
    for k in range(n_dev):
        part_ref[k] = part[k * rows : (k + 1) * rows, :]
    take_ref[me] = part_ref[me]
    copies = []
    for r, peer in peers.items():
        pid = peer[0] * ep_size + peer[1]
        copies.append(pltpu.make_async_remote_copy(src_ref=part_ref.at[pid], dst_ref=take_ref.at[me], send_sem=sem_c.at[r], recv_sem=sem_d.at[r], device_id=peer, device_id_type=MESH))
        copies[-1].start()
    for c in copies:
        c.wait()
    total = take_ref[0]
    for k in range(1, n_dev):
        total = total + take_ref[k]
    gr_ref[me] = total
    copies = []
    for r, peer in peers.items():
        copies.append(pltpu.make_async_remote_copy(src_ref=gr_ref.at[me], dst_ref=gr_ref.at[me], send_sem=sem_e.at[r], recv_sem=sem_f.at[r], device_id=peer, device_id_type=MESH))
        copies[-1].start()
    for c in copies:
        c.wait()


def router_backward(dg, gates, tokens, n_dev, ep_size):
    n_exp = gates.shape[0] * gates.shape[1]
    n_tok, hidden = tokens.shape
    vmem = pl.BlockSpec(memory_space=pltpu.VMEM)
    rows = n_exp // n_dev
    dma = pltpu.SemaphoreType.DMA((n_dev,))
    return pl.pallas_call(
        functools.partial(router_kernel, n_dev=n_dev, ep_size=ep_size),
        out_shape=[jax.ShapeDtypeStruct((n_exp, n_tok), BF16), jax.ShapeDtypeStruct((n_dev, rows, hidden), F32)],
        in_specs=[vmem] * 3,
        out_specs=[vmem] * 2,
        scratch_shapes=[
            pltpu.VMEM((ep_size, n_exp // ep_size, n_tok), F32),
            pltpu.VMEM((n_dev, rows, hidden), F32),
            pltpu.VMEM((n_dev, rows, hidden), F32),
            *([dma] * 6),
        ],
        compiler_params=pltpu.CompilerParams(collective_id=1, has_side_effects=True),
        cost_estimate=pl.CostEstimate(flops=2_000_000_000, bytes_accessed=2_000_000, transcendentals=0),
        name='router_backward',
    )(dg, gates, tokens)


def _slots(g_ref, start_ref, slot_ref):
    tri = (lax.broadcasted_iota(I32, (BLK, BLK), 0) < lax.broadcasted_iota(I32, (BLK, BLK), 1)).astype(F32).astype(BF16)
    sel = g_ref[...] >= 0.0
    pos = _dot(jnp.where(sel, 1.0, 0.0).astype(BF16), tri, 1, 0).astype(I32)
    slot_ref[...] = jnp.where(sel, pos + start_ref[...], -1)


def _onehot(code_ref, i, k, slot_ref, g_ref, hot_ref, gate_ref, n_exp):
    for q in range(PER):
        code = code_ref[i, k * PER + q]
        e = lax.rem(code, GRP)
        ids = lax.broadcasted_iota(I32, (GRP, BLK), 0) + (k * STEP + q * GRP)
        at = pl.ds(i * n_exp + e, 1)
        eq = slot_ref[at, :] == ids
        rows = slice(q * GRP, (q + 1) * GRP)
        hot_ref[rows, :] = jnp.where(eq, 1.0, 0.0).astype(BF16)
        gate_ref[rows, :] = jnp.where(eq, g_ref[at, :], 0.0)


def sort_kernel(meta_ref, code_ref, zero_ref, g_ref, start_ref, *rest, n_exp, n_blk, skip):
    srcs = rest[:n_blk]
    out_ref, slot_ref, x_ref, buf_ref, zbuf_ref, hot_ref, gate_ref, xsem, sem_ref, zsem = rest[n_blk:]
    hidden = x_ref.shape[2] // 2

    def zeros(q):
        return pltpu.make_async_copy(zbuf_ref, out_ref.at[pl.ds(pl.multiple_of(q * GRP, GRP), GRP), :], zsem.at[0])

    for k in range(n_blk):
        pltpu.make_async_copy(srcs[k], x_ref.at[k], xsem.at[k]).start()
    zbuf_ref[...] = jnp.zeros_like(zbuf_ref)
    for e in range(n_exp):
        lax.fori_loop(0, zero_ref[1, e], lambda q, c: (zeros(zero_ref[0, e] + q).start(), c)[1], 0)
    _slots(g_ref, start_ref, slot_ref)

    def drain(s, cnt):
        @pl.when(cnt == PER)
        def _():
            pltpu.make_async_copy(buf_ref.at[0], out_ref.at[pl.ds(0, STEP), :], sem_ref.at[s]).wait()

        @pl.when(cnt < PER)
        def _():
            def one(_, c):
                pltpu.make_async_copy(buf_ref.at[0, pl.ds(0, GRP), :], out_ref.at[pl.ds(0, GRP), :], sem_ref.at[s]).wait()
                return c

            lax.fori_loop(0, cnt, one, 0)

    def block(i, c):
        n_grp = meta_ref[skip + i]
        pltpu.make_async_copy(srcs[0], x_ref.at[i], xsem.at[i]).wait()

        def step(k, c):
            s, old, newer = c
            _onehot(code_ref, skip + i, k, slot_ref, g_ref, hot_ref, gate_ref, n_exp)
            gcol = jnp.sum(gate_ref[...], axis=1, keepdims=True)
            hot = hot_ref[...]
            drain(s, old)
            buf_ref[s, :, :hidden] = _dot(hot, x_ref[i, :, :hidden], 1, 0).astype(BF16)
            buf_ref[s, :, hidden:] = (gcol * _dot(hot, x_ref[i, :, hidden:], 1, 0)).astype(BF16)
            cnt = jnp.minimum(n_grp - k * PER, PER)

            def send(q, c):
                code = code_ref[skip + i, k * PER + q]
                dst = pl.multiple_of(code - lax.rem(code, GRP), GRP)
                pltpu.make_async_copy(buf_ref.at[s, pl.ds(pl.multiple_of(q * GRP, GRP), GRP), :], out_ref.at[pl.ds(dst, GRP), :], sem_ref.at[s]).start()
                return c

            @pl.when(cnt == PER)
            def _():
                for q in range(PER):
                    send(q, 0)

            @pl.when(cnt < PER)
            def _():
                lax.fori_loop(0, cnt, send, 0)

            return 1 - s, newer, cnt

        return lax.fori_loop(0, (n_grp + PER - 1) // PER, step, c)

    s, old, newer = lax.fori_loop(0, n_blk, block, (jnp.int32(0), jnp.int32(0), jnp.int32(0)))
    drain(s, old)
    drain(1 - s, newer)
    for e in range(n_exp):
        lax.fori_loop(0, zero_ref[1, e], lambda q, c: (zeros(0).wait(), c)[1], 0)


def sort_rows(meta, code, zero, gates, start, blocks, skip, rows, n_exp):
    n_blk = len(blocks)
    width = blocks[0].shape[1]
    smem = pl.BlockSpec(memory_space=pltpu.SMEM)
    vmem = pl.BlockSpec(memory_space=pltpu.VMEM)
    hbm = pl.BlockSpec(memory_space=pl.ANY)
    return pl.pallas_call(
        functools.partial(sort_kernel, n_exp=n_exp, n_blk=n_blk, skip=skip),
        out_shape=jax.ShapeDtypeStruct((rows, width), BF16),
        in_specs=[smem] * 3 + [vmem] * 2 + [hbm] * n_blk,
        out_specs=hbm,
        scratch_shapes=[
            pltpu.VMEM(gates.shape, I32),
            pltpu.VMEM((n_blk, BLK, width), BF16),
            pltpu.VMEM((2, STEP, width), BF16),
            pltpu.VMEM((GRP, width), BF16),
            pltpu.VMEM((STEP, BLK), BF16),
            pltpu.VMEM((STEP, BLK), F32),
            pltpu.SemaphoreType.DMA((n_blk,)),
            pltpu.SemaphoreType.DMA((2,)),
            pltpu.SemaphoreType.DMA((1,)),
        ],
        cost_estimate=pl.CostEstimate(flops=1_500_000_000 * n_blk, bytes_accessed=3_000_000 * n_blk, transcendentals=0),
    )(meta, code, zero, gates, start, *blocks)


def _units(first, n, src_ref, buf_ref, sem, slot, op):
    for j in range(MOST):

        @pl.when(j < n)
        def _():
            row = pl.multiple_of((first + j) * UNIT, UNIT)
            op(pltpu.make_async_copy(src_ref.at[pl.ds(row, UNIT), :], buf_ref.at[slot, pl.ds(j * UNIT, UNIT), :], sem.at[slot]))


def _start(c):
    c.start()


def _wait(c):
    c.wait()


def _piece(n, k):
    cuts = (n + MOST - 1) // MOST
    low = n // cuts
    extra = n - low * cuts
    return k * low + jnp.minimum(k, extra), low + jnp.where(k < extra, 1, 0), cuts


def _next(t_ref, e, k, cuts, n_exp):
    here = _piece(t_ref[1, e], jnp.minimum(k + 1, cuts - 1))[1]
    there = jnp.where(e + 1 < n_exp, _piece(t_ref[1, jnp.minimum(e + 1, n_exp - 1)], 0)[1], 0)
    return jnp.where(k + 1 < cuts, here, there)


def _hidden(u, d, w1_ref, w3_ref, w2_ref, j, w):
    h1 = _dot(u, w1_ref[0, :, j : j + w], 1, 0)
    h3 = _dot(u, w3_ref[0, :, j : j + w], 1, 0)
    da = _dot(d, w2_ref[0, j : j + w, :], 1, 1)
    sig = jax.nn.sigmoid(h1)
    silu = h1 * sig
    act = (silu * h3).astype(BF16)
    dh1 = (da * h3 * sig * (1.0 + h1 * (1.0 - sig))).astype(BF16)
    dh3 = (da * silu).astype(BF16)
    return act, dh1, dh3


def own_kernel(t_ref, ud_ref, w1_ref, w3_ref, w2_ref, o_ref, sv_ref, in_ref, ob_ref, sb_ref, cnt_ref, isem, osem, ssem, *, n_exp, hidden, inner):
    e = pl.program_id(0)

    def put(g, n, s, op):
        for j in range(MOST):

            @pl.when(j < n)
            def _():
                rows = pl.ds(pl.multiple_of((g + j) * UNIT, UNIT), UNIT)
                op(pltpu.make_async_copy(ob_ref.at[s, pl.ds(j * UNIT, UNIT), :], o_ref.at[rows, :], osem.at[s]))
                op(pltpu.make_async_copy(sb_ref.at[s, pl.ds(j * UNIT, UNIT), :], sv_ref.at[rows, :], ssem.at[s]))

    @pl.when(e == 0)
    def _():
        cnt_ref[0] = 0
        cnt_ref[1] = 0
        cnt_ref[2] = 0
        _units(0, _piece(t_ref[1, 0], 0)[1], ud_ref, in_ref, isem, 0, _start)

    def piece(k, c):
        off, n, cuts = _piece(t_ref[1, e], k)
        g = t_ref[0, e] + off
        s = lax.rem(cnt_ref[2], 2)
        cnt_ref[2] = cnt_ref[2] + 1
        _units(g, n, ud_ref, in_ref, isem, s, _wait)
        _units(g + n, _next(t_ref, e, k, cuts, n_exp), ud_ref, in_ref, isem, 1 - s, _start)
        put(0, cnt_ref[s], s, _wait)
        cnt_ref[s] = n
        for size in range(1, MOST + 1):

            @pl.when(n == size)
            def _():
                r = size * UNIT
                for j in range(0, inner, 256):
                    act, dh1, dh3 = _hidden(in_ref[s, :r, :hidden], in_ref[s, :r, hidden:], w1_ref, w3_ref, w2_ref, j, 256)
                    sb_ref[s, :r, j : j + 256] = act
                    sb_ref[s, :r, inner + j : inner + j + 256] = dh1
                    sb_ref[s, :r, 2 * inner + j : 2 * inner + j + 256] = dh3
                ob_ref[s, :r, :hidden] = _dot(sb_ref[s, :r, :inner], w2_ref[0], 1, 0).astype(BF16)
                ob_ref[s, :r, hidden:] = (_dot(sb_ref[s, :r, inner : 2 * inner], w1_ref[0], 1, 1) + _dot(sb_ref[s, :r, 2 * inner :], w3_ref[0], 1, 1)).astype(BF16)

        put(g, n, s, _start)
        return c

    lax.fori_loop(0, (t_ref[1, e] + MOST - 1) // MOST, piece, 0)

    @pl.when(e == n_exp - 1)
    def _():
        for s in range(2):
            put(0, cnt_ref[s], s, _wait)


def own_rows(table, ud, w1, w3, w2):
    n_exp, hidden, inner = w1.shape
    n_row, width = ud.shape
    wspec = lambda a, b: pl.BlockSpec((1, a, b), lambda e, t: (e, 0, 0))
    hbm = pl.BlockSpec(memory_space=pl.ANY)
    spec = pltpu.PrefetchScalarGridSpec(
        num_scalar_prefetch=1,
        grid=(n_exp,),
        in_specs=[hbm, wspec(hidden, inner), wspec(hidden, inner), wspec(inner, hidden)],
        out_specs=[hbm, hbm],
        scratch_shapes=[
            pltpu.VMEM((2, MOST * UNIT, width), BF16),
            pltpu.VMEM((2, MOST * UNIT, width), BF16),
            pltpu.VMEM((2, MOST * UNIT, 3 * inner), BF16),
            pltpu.SMEM((3,), I32),
            pltpu.SemaphoreType.DMA((2,)),
            pltpu.SemaphoreType.DMA((2,)),
            pltpu.SemaphoreType.DMA((2,)),
        ],
    )
    return pl.pallas_call(
        functools.partial(own_kernel, n_exp=n_exp, hidden=hidden, inner=inner),
        out_shape=[jax.ShapeDtypeStruct((n_row, width), BF16), jax.ShapeDtypeStruct((n_row, 3 * inner), BF16)],
        grid_spec=spec,
        name='own_rows',
        cost_estimate=pl.CostEstimate(flops=30_000_000_000, bytes_accessed=60_000_000, transcendentals=2_000_000),
    )(table, ud, w1, w3, w2)


def grads_kernel(ta_ref, tb_ref, uo_ref, sv_ref, ud_ref, w1_ref, w3_ref, w2_ref, g1_ref, g3_ref, g2_ref, oin_ref, sin_ref, in_ref, act_ref, dh_ref, cnt_ref, osem, ssem, isem, *, n_exp, hidden, inner):
    e = pl.program_id(0)

    @pl.when(e == 0)
    def _():
        cnt_ref[0] = 0
        cnt_ref[1] = 0
        n = _piece(ta_ref[1, 0], 0)[1]
        _units(0, n, uo_ref, oin_ref, osem, 0, _start)
        _units(0, n, sv_ref, sin_ref, ssem, 0, _start)
        _units(0, _piece(tb_ref[1, 0], 0)[1], ud_ref, in_ref, isem, 0, _start)

    mc = 256

    def outer(x_ref, s, r, act, dh1, dh3, fresh):
        def put(ref, m, v):
            ref[0, m : m + mc, :] = v if fresh else ref[0, m : m + mc, :] + v

        for m in range(0, hidden, mc):
            u = x_ref[s, :r, m : m + mc]
            put(g1_ref, m, _dot(u, dh1, 0, 0))
            put(g3_ref, m, _dot(u, dh3, 0, 0))
        d = x_ref[s, :r, hidden:]
        for m in range(0, inner, mc):
            put(g2_ref, m, _dot(act[:, m : m + mc], d, 0, 0))

    def own_piece(k, c):
        off, n, cuts = _piece(ta_ref[1, e], k)
        g = ta_ref[0, e] + off
        s = lax.rem(cnt_ref[0], 2)
        cnt_ref[0] = cnt_ref[0] + 1
        _units(g, n, uo_ref, oin_ref, osem, s, _wait)
        _units(g, n, sv_ref, sin_ref, ssem, s, _wait)
        m = _next(ta_ref, e, k, cuts, n_exp)
        _units(g + n, m, uo_ref, oin_ref, osem, 1 - s, _start)
        _units(g + n, m, sv_ref, sin_ref, ssem, 1 - s, _start)
        for size, fresh in [(v, True) for v in range(1, MOST + 1)] + [(v, False) for v in range(2, MOST + 1)]:

            @pl.when(jnp.logical_and(n == size, (k == 0) == fresh))
            def _():
                r = size * UNIT
                outer(oin_ref, s, r, sin_ref[s, :r, :inner], sin_ref[s, :r, inner : 2 * inner], sin_ref[s, :r, 2 * inner :], fresh)

        return c

    lax.fori_loop(0, (ta_ref[1, e] + MOST - 1) // MOST, own_piece, 0)

    def piece(k, c):
        off, n, cuts = _piece(tb_ref[1, e], k)
        g = tb_ref[0, e] + off
        s = lax.rem(cnt_ref[1], 2)
        cnt_ref[1] = cnt_ref[1] + 1
        _units(g, n, ud_ref, in_ref, isem, s, _wait)
        _units(g + n, _next(tb_ref, e, k, cuts, n_exp), ud_ref, in_ref, isem, 1 - s, _start)
        for size in range(1, MOST + 1):

            @pl.when(n == size)
            def _():
                r = size * UNIT
                for j in range(0, inner, mc):
                    act, dh1, dh3 = _hidden(in_ref[s, :r, :hidden], in_ref[s, :r, hidden:], w1_ref, w3_ref, w2_ref, j, mc)
                    act_ref[:r, j : j + mc] = act
                    dh_ref[:r, j : j + mc] = dh1
                    dh_ref[:r, inner + j : inner + j + mc] = dh3
                outer(in_ref, s, r, act_ref[:r, :], dh_ref[:r, :inner], dh_ref[:r, inner:], False)

        return c

    lax.fori_loop(0, (tb_ref[1, e] + MOST - 1) // MOST, piece, 0)


def weight_grads(ta, tb, uo, sv, ud, w1, w3, w2):
    n_exp, hidden, inner = w1.shape
    width = ud.shape[1]
    wspec = lambda a, b: pl.BlockSpec((1, a, b), lambda e, t, s: (e, 0, 0))
    hbm = pl.BlockSpec(memory_space=pl.ANY)
    most = MOST * UNIT
    spec = pltpu.PrefetchScalarGridSpec(
        num_scalar_prefetch=2,
        grid=(n_exp,),
        in_specs=[hbm, hbm, hbm, wspec(hidden, inner), wspec(hidden, inner), wspec(inner, hidden)],
        out_specs=[wspec(hidden, inner), wspec(hidden, inner), wspec(inner, hidden)],
        scratch_shapes=[
            pltpu.VMEM((2, most, width), BF16),
            pltpu.VMEM((2, most, 3 * inner), BF16),
            pltpu.VMEM((2, most, width), BF16),
            pltpu.VMEM((most, inner), BF16),
            pltpu.VMEM((most, 2 * inner), BF16),
            pltpu.SMEM((2,), I32),
            pltpu.SemaphoreType.DMA((2,)),
            pltpu.SemaphoreType.DMA((2,)),
            pltpu.SemaphoreType.DMA((2,)),
        ],
    )
    return pl.pallas_call(
        functools.partial(grads_kernel, n_exp=n_exp, hidden=hidden, inner=inner),
        out_shape=[jax.ShapeDtypeStruct(w.shape, F32) for w in (w1, w3, w2)],
        grid_spec=spec,
        name='weight_grads',
        cost_estimate=pl.CostEstimate(flops=90_000_000_000, bytes_accessed=150_000_000, transcendentals=4_000_000),
    )(ta, tb, uo, sv, ud, w1, w3, w2)


def combine_kernel(meta_ref, code_ref, g_ref, start_ref, r_ref_a, r_ref_b, o_ref, *rest, n_exp, hidden, which, more):
    if more:
        add_ref, keep_ref, go_ref, dg_ref, p_ref, slot_ref, buf_ref, hot_ref, gate_ref, sem_ref = rest
    else:
        p_ref, dg_ref, slot_ref, buf_ref, hot_ref, gate_ref, sem_ref = rest
    i = pl.program_id(0)

    def rel(k):
        return which[0] + k * (which[1] - which[0])

    def pull(k, s):
        def one(q, c):
            code = code_ref[rel(k), q]
            src = pl.multiple_of(code - lax.rem(code, GRP), GRP)
            pltpu.make_async_copy(o_ref.at[pl.ds(src, GRP), :], buf_ref.at[s, pl.ds(pl.multiple_of(q * GRP, GRP), GRP), :], sem_ref.at[s]).start()
            return c

        lax.fori_loop(0, meta_ref[rel(k)], one, 0)

    @pl.when(i == 0)
    def _():
        pull(0, 0)
        pull(1, 1)
        _slots(g_ref, start_ref, slot_ref)

    n_grp = meta_ref[rel(i)]
    n_step = (n_grp + PER - 1) // PER

    def blank(q, c):
        buf_ref[i, pl.ds(pl.multiple_of(q * GRP, GRP), GRP), :] = jnp.zeros((GRP, buf_ref.shape[2]), BF16)
        return c

    lax.fori_loop(n_grp, n_step * PER, blank, 0)
    if more:
        p_ref[...] = add_ref[...]
    else:
        p_ref[...] = jnp.zeros_like(p_ref)
    dg_ref[...] = jnp.zeros_like(dg_ref)

    def whole(q, c):
        pltpu.make_async_copy(o_ref.at[pl.ds(0, STEP), :], buf_ref.at[0, pl.ds(0, STEP), :], sem_ref.at[i]).wait()
        return c

    def single(q, c):
        pltpu.make_async_copy(o_ref.at[pl.ds(0, GRP), :], buf_ref.at[0, pl.ds(0, GRP), :], sem_ref.at[i]).wait()
        return c

    lax.fori_loop(0, n_grp // PER, whole, 0)
    lax.fori_loop(0, lax.rem(n_grp, PER), single, 0)

    def step(k, c):
        rows = pl.ds(pl.multiple_of(k * STEP, STEP), STEP)
        o = buf_ref[i, rows, :hidden]
        rg = buf_ref[i, rows, hidden:]
        prod = _dot(o, jnp.where(i == 0, r_ref_a[...], r_ref_b[...]), 1, 1)
        _onehot(code_ref, rel(i), k, slot_ref, g_ref, hot_ref, gate_ref, n_exp)
        hot = hot_ref[...]
        prod = jnp.where(hot.astype(F32) > 0.5, prod, 0.0)
        for q in range(PER):
            e = lax.rem(code_ref[rel(i), k * PER + q], GRP)
            dg_ref[0, pl.ds(e, 1), :] += jnp.sum(prod[q * GRP : (q + 1) * GRP, :], axis=0, keepdims=True)
        gsel = gate_ref[...]
        g_hi = gsel.astype(BF16)
        rest = gsel - g_hi.astype(F32)
        g_mid = rest.astype(BF16)
        g_lo = (rest - g_mid.astype(F32)).astype(BF16)
        p_ref[:, :hidden] += _dot(g_hi, o, 0, 0) + (_dot(g_mid, o, 0, 0) + _dot(g_lo, o, 0, 0))
        p_ref[:, hidden:] += _dot(hot, rg, 0, 0)
        return c

    lax.fori_loop(0, n_step, step, 0)
    if more:

        @pl.when(i == 0)
        def _():
            keep_ref[...] = p_ref[...]

        @pl.when(i == 1)
        def _():
            go_ref[...] = p_ref[...]


def combine(meta, code, gates, start, blocks, o_rows, which, n_exp, add=None):
    width = o_rows.shape[1]
    hidden = width // 2
    half = pl.BlockSpec((BLK, hidden), lambda i, m, s: (0, 1))
    block = pl.BlockSpec((BLK, width), lambda i, m, s: (i, 0))
    more = [] if add is None else [add]
    whole = pl.BlockSpec(gates.shape, lambda i, m, s: (0, 0))
    fixed = pl.BlockSpec((BLK, width), lambda i, m, s: (0, 0))
    spec = pltpu.PrefetchScalarGridSpec(
        num_scalar_prefetch=2,
        grid=(2,),
        in_specs=[
            whole,
            whole,
            half,
            half,
            pl.BlockSpec(memory_space=pl.ANY),
            *([block] * len(more)),
        ],
        out_specs=([fixed] * 2 if more else [block]) + [pl.BlockSpec((1, n_exp, BLK), lambda i, m, s: (i, 0, 0))],
        scratch_shapes=[
            *([pltpu.VMEM((BLK, width), F32)] * len(more)),
            pltpu.VMEM(gates.shape, I32),
            pltpu.VMEM((2, BLK * n_exp, width), BF16),
            pltpu.VMEM((STEP, BLK), BF16),
            pltpu.VMEM((STEP, BLK), F32),
            pltpu.SemaphoreType.DMA((2,)),
        ],
    )
    return pl.pallas_call(
        functools.partial(combine_kernel, n_exp=n_exp, hidden=hidden, which=which, more=bool(more)),
        out_shape=([jax.ShapeDtypeStruct((BLK, width), F32)] * 2 if more else [jax.ShapeDtypeStruct((2 * BLK, width), F32)]) + [jax.ShapeDtypeStruct((2, n_exp, BLK), F32)],
        grid_spec=spec,
        name='combine',
        cost_estimate=pl.CostEstimate(flops=8_000_000_000, bytes_accessed=20_000_000, transcendentals=0),
    )(meta, code, gates, start, blocks[which[0]], blocks[which[1]], o_rows, *more)


def routing_tables(cnt, n_own):
    n_blk, n_exp = cnt.shape
    pad = (cnt + GRP - 1) // GRP * GRP
    before_e = (jnp.arange(n_exp)[:, None] < jnp.arange(n_exp)[None, :]).astype(I32)
    blk = jnp.arange(n_blk)
    same = (blk[:, None] < n_own) == (blk[None, :] < n_own)
    before_b = ((blk[:, None] < blk[None, :]) & same).astype(I32)
    blk_start = jnp.sum(pad[:, :, None] * before_e[None], axis=1)
    blk_end = blk_start + pad
    in_exp = jnp.sum(pad[:, None, :] * before_b[:, :, None], axis=0)

    def part(p):
        total = jnp.sum(p, axis=0)
        units = jnp.maximum((total + UNIT - 1) // UNIT, 1)
        first = jnp.sum(units[:, None] * before_e, axis=0)
        zero = jnp.stack([(first * UNIT + total) // GRP, (units * UNIT - total) // GRP])
        return jnp.stack([first, units]).astype(I32), zero.astype(I32), first * UNIT

    ta, za, base_a = part(pad[:n_own])
    tb, zb, base_b = part(pad[n_own:])
    base = jnp.where(blk[:, None] < n_own, base_a[None], base_b[None])
    q = jnp.arange(BLK * n_exp // GRP, dtype=I32) * GRP
    inside = (q[None, :, None] >= blk_start[:, None, :]) & (q[None, :, None] < blk_end[:, None, :])
    place = base + in_exp - blk_start + jnp.arange(n_exp, dtype=I32)[None]
    code = jnp.sum(jnp.where(inside, place[:, None, :] + q[None, :, None], 0), axis=2)
    start = jnp.broadcast_to(blk_start.reshape(n_blk * n_exp, 1), (n_blk * n_exp, BLK)).astype(I32)
    return (jnp.sum(pad, axis=1) // GRP).astype(I32), start, code.astype(I32), ta, za, tb, zb


def solution(mesh):
    ep_size = mesh.shape['ep']
    dp_size = mesh.shape['dp']
    n_dev = ep_size * dp_size
    all_axes = ('dp', 'ep')

    def swap(v, mask):
        return lax.ppermute(v, all_axes, [(d, d ^ mask) for d in range(n_dev)])

    def layer(tokens, w_router, w_gate, w_up, w_down, top_ids, r_proj):
        n_local, hidden = tokens.shape
        n_exp = w_router.shape[1]
        local_exp = w_gate.shape[0]
        xr = jnp.concatenate([tokens, r_proj], axis=1)
        blk = {0: xr}
        own_gates, gates, *got = first_stage(tokens, w_router, top_ids.T, xr, n_dev, ep_size)
        blk.update(zip((1, 2, 4, 8, 3, 5, 9), got))
        for dst, src, mask in ((6, 4, 2), (12, 8, 4), (10, 2, 8)):
            blk[dst] = swap(blk[src], mask)
        cnt = jnp.sum((gates >= 0).astype(I32), axis=2)
        gates = gates.reshape(n_dev * local_exp, n_local)
        meta, start, code, ta, za, tb, zb = routing_tables(cnt, ep_size)
        own_n = ep_size * n_local * local_exp + local_exp * UNIT
        oth_n = (n_dev - ep_size) * n_local * local_exp + local_exp * UNIT
        uo = sort_rows(meta, code, za, gates, start, [blk[k] for k in range(4)], 0, own_n, local_exp)
        o_rows, sv = own_rows(ta, uo, w_gate, w_up, w_down)
        p_send, dg_b = combine(meta, code, gates, start, blk, o_rows, (1, 3), local_exp)
        p_sib = swap(p_send, 1)
        late = [blk[6], blk[10], blk[12]]
        p_send, *late = lax.optimization_barrier((p_send, *late))
        blk[6], blk[10], blk[12] = late
        blk[7], blk[11], blk[13], blk[14], blk[15] = last_stage(*late, n_dev, ep_size)
        ud = sort_rows(meta, code, zb, gates, start, [blk[k] for k in range(4, 16)], 4, oth_n, local_exp)
        p_sib, ud = lax.optimization_barrier((p_sib, ud))
        p_keep, p_go, dg_a = combine(meta, code, gates, start, blk, o_rows, (0, 2), local_exp, p_sib)
        dg = jnp.stack([dg_a[0], dg_b[0], dg_a[1], dg_b[1]])
        dz_t, grad_router_t = router_backward(dg, own_gates, tokens, n_dev, ep_size)
        p_go, dz_t = lax.optimization_barrier((p_go, dz_t))
        p_far = swap(p_go, 2)
        g_gate, g_up, g_down = weight_grads(ta, tb, uo, sv, ud, w_gate, w_up, w_down)
        grad_router = grad_router_t.reshape(n_exp, hidden).T
        y = tokens.astype(F32) + (p_keep[:, :hidden] + p_far[:, :hidden])
        dx = r_proj.astype(F32) + _dot(dz_t, w_router, 0, 1) + (p_keep[:, hidden:] + p_far[:, hidden:])
        return y, dx, g_gate, g_up, g_down, grad_router

    tok_spec = P(all_axes, None)
    exp_spec = P('ep', None, None)
    return jax.shard_map(layer, mesh=mesh, in_specs=(tok_spec, P(), exp_spec, exp_spec, exp_spec, tok_spec, tok_spec), out_specs=(tok_spec, tok_spec, exp_spec, exp_spec, exp_spec, P()), check_vma=False)
```

```python
import functools

import jax
import jax.numpy as jnp
from jax import lax
from jax.experimental import pallas as pl
from jax.experimental.pallas import tpu as pltpu
from jax.sharding import PartitionSpec as P


F32 = jnp.float32
BF16 = jnp.bfloat16
I32 = jnp.int32
GRP = 16
UNIT = 128
MOST = 4
STEP = 256
BLK = 256
PER = STEP // GRP
MESH = pl.DeviceIdType.MESH


def _dot(a, b, ca, cb):
    return lax.dot_general(a, b, (((ca,), (cb,)), ((), ())), preferred_element_type=F32)


def _flip(v, mask):
    for k in range(2):
        if (mask >> k) & 1:
            v = v + (1 << k) * (1 - 2 * ((v // (1 << k)) % 2))
    return v


def _peers(dp, ep, ep_size, n_dev):
    return {r: (_flip(dp, r // ep_size), _flip(ep, r % ep_size)) for r in range(1, n_dev)}


def _greet(peers):
    barrier = pltpu.get_barrier_semaphore()
    for peer in peers.values():
        pl.semaphore_signal(barrier, inc=1, device_id=peer, device_id_type=MESH)
    pl.semaphore_wait(barrier, len(peers))


def first_kernel(x_ref, wr_ref, ids_ref, xr_ref, own_ref, out_ref, b1, b2, b4, b8, b3, b5, b9, ssem, rsem, bsend, brecv, fsend, frecv, *, n_dev, ep_size):
    dp, ep = lax.axis_index('dp'), lax.axis_index('ep')
    peers = _peers(dp, ep, ep_size, n_dev)
    local = out_ref.shape[1]
    _greet(peers)

    def copy(src, dst, s, r, k, mask):
        return pltpu.make_async_remote_copy(src_ref=src, dst_ref=dst, send_sem=s.at[k], recv_sem=r.at[k], device_id=peers[mask], device_id_type=MESH)

    half = xr_ref.shape[0] // 2
    part = [pl.ds(0, half), pl.ds(half, half)]
    direct = []
    for h in range(2):
        for k, (dst, mask) in enumerate(((b2, 2), (b4, 4), (b8, 8), (b1, 1))):
            direct.append(copy(xr_ref.at[part[h], :], dst.at[part[h], :], bsend, brecv, 4 * h + k, mask))
    for c in direct[:4]:
        c.start()
    z = _dot(wr_ref[...], x_ref[...], 1, 1)
    eid = lax.broadcasted_iota(I32, z.shape, 0)
    sel = eid == ids_ref[0:1, :]
    for j in range(1, ids_ref.shape[0]):
        sel = jnp.logical_or(sel, eid == ids_ref[j : j + 1, :])
    peak = jnp.max(jnp.where(sel, z, -3.0e38), axis=0, keepdims=True)
    ex = jnp.where(sel, jnp.exp(jnp.where(sel, z - peak, 0.0)), 0.0)
    gates = ex / jnp.sum(ex, axis=0, keepdims=True)
    marked = jnp.where(sel, gates, -1.0)
    for k in range(ep_size):
        own_ref[k] = marked[k * local : (k + 1) * local, :]
    out_ref[0] = own_ref[ep]
    direct[3].wait_recv()
    small = [copy(own_ref.at[peer[1]], out_ref.at[r], ssem, rsem, r, r) for r, peer in peers.items()]
    for c in small + direct[4:]:
        c.start()
    passed = []
    for h in range(2):
        for k, (src, dst) in enumerate(((b2, b3), (b4, b5), (b8, b9))):
            direct[4 * h + k].wait_recv()
            passed.append(copy(src.at[part[h], :], dst.at[part[h], :], fsend, frecv, 3 * h + k, 1))
            passed[-1].start()
    direct[7].wait_recv()
    for c in direct:
        c.wait_send()
    for c in passed + small:
        c.wait()


def first_stage(tokens, w_router, ids_t, xr, n_dev, ep_size):
    local = w_router.shape[0] // ep_size
    n_tok = tokens.shape[0]
    vmem = pl.BlockSpec(memory_space=pltpu.VMEM)
    hbm = pl.BlockSpec(memory_space=pl.ANY)
    dma = pltpu.SemaphoreType.DMA
    return pl.pallas_call(
        functools.partial(first_kernel, n_dev=n_dev, ep_size=ep_size),
        out_shape=[jax.ShapeDtypeStruct((ep_size, local, n_tok), F32), jax.ShapeDtypeStruct((n_dev, local, n_tok), F32)] + [jax.ShapeDtypeStruct(xr.shape, BF16)] * 7,
        in_specs=[vmem] * 3 + [hbm],
        out_specs=[vmem] * 2 + [hbm] * 7,
        scratch_shapes=[dma((n_dev,)), dma((n_dev,)), dma((8,)), dma((8,)), dma((6,)), dma((6,))],
        compiler_params=pltpu.CompilerParams(collective_id=0, has_side_effects=True),
        cost_estimate=pl.CostEstimate(flops=20_000_000_000, bytes_accessed=20_000_000, transcendentals=0),
        name='first_stage',
    )(tokens, w_router, ids_t, xr)


def router_kernel(dg_ref, g_ref, x_ref, dz_ref, out_ref, gr_ref, all_ref, part_ref, take_ref, sem_a, sem_b, sem_c, sem_d, sem_e, sem_f, *, n_dev, ep_size):
    dp, ep = lax.axis_index('dp'), lax.axis_index('ep')
    me = dp * ep_size + ep
    peers = _peers(dp, ep, ep_size, n_dev)
    all_ref[ep] = dg_ref[0]
    _greet(peers)
    copies = []
    for r in range(1, ep_size):
        copies.append(pltpu.make_async_remote_copy(src_ref=dg_ref.at[r], dst_ref=all_ref.at[ep], send_sem=sem_a.at[r], recv_sem=sem_b.at[r], device_id=peers[r], device_id_type=MESH))
        copies[-1].start()
    for c in copies:
        c.wait()
    g = jnp.maximum(jnp.concatenate([g_ref[k] for k in range(ep_size)], axis=0), 0.0)
    dg = jnp.concatenate([all_ref[k] for k in range(ep_size)], axis=0)
    dz = (g * (dg - jnp.sum(g * dg, axis=0, keepdims=True))).astype(BF16)
    dz_ref[...] = dz
    part = _dot(dz, x_ref[...], 1, 0)
    rows = part.shape[0] // n_dev
    for k in range(n_dev):
        part_ref[k] = part[k * rows : (k + 1) * rows, :]
    take_ref[me] = part_ref[me]
    copies = []
    for r, peer in peers.items():
        pid = peer[0] * ep_size + peer[1]
        copies.append(pltpu.make_async_remote_copy(src_ref=part_ref.at[pid], dst_ref=take_ref.at[me], send_sem=sem_c.at[r], recv_sem=sem_d.at[r], device_id=peer, device_id_type=MESH))
        copies[-1].start()
    for c in copies:
        c.wait()
    total = take_ref[0]
    for k in range(1, n_dev):
        total = total + take_ref[k]
    gr_ref[me] = total
    copies = []
    for r, peer in peers.items():
        copies.append(pltpu.make_async_remote_copy(src_ref=gr_ref.at[me], dst_ref=gr_ref.at[me], send_sem=sem_e.at[r], recv_sem=sem_f.at[r], device_id=peer, device_id_type=MESH))
        copies[-1].start()
    for c in copies:
        c.wait()
    out_ref[...] = jnp.concatenate([gr_ref[k] for k in range(n_dev)], axis=0)


def router_backward(dg, gates, tokens, n_dev, ep_size):
    n_exp = gates.shape[0] * gates.shape[1]
    n_tok, hidden = tokens.shape
    vmem = pl.BlockSpec(memory_space=pltpu.VMEM)
    rows = n_exp // n_dev
    dma = pltpu.SemaphoreType.DMA((n_dev,))
    return pl.pallas_call(
        functools.partial(router_kernel, n_dev=n_dev, ep_size=ep_size),
        out_shape=[jax.ShapeDtypeStruct((n_exp, n_tok), BF16), jax.ShapeDtypeStruct((n_exp, hidden), F32)],
        in_specs=[vmem] * 3,
        out_specs=[vmem] * 2,
        scratch_shapes=[
            pltpu.VMEM((n_dev, rows, hidden), F32),
            pltpu.VMEM((ep_size, n_exp // ep_size, n_tok), F32),
            pltpu.VMEM((n_dev, rows, hidden), F32),
            pltpu.VMEM((n_dev, rows, hidden), F32),
            *([dma] * 6),
        ],
        compiler_params=pltpu.CompilerParams(collective_id=1, has_side_effects=True),
        cost_estimate=pl.CostEstimate(flops=2_000_000_000, bytes_accessed=2_000_000, transcendentals=0),
        name='router_backward',
    )(dg, gates, tokens)


def _slots(g_ref, start_ref, slot_ref):
    tri = (lax.broadcasted_iota(I32, (BLK, BLK), 0) < lax.broadcasted_iota(I32, (BLK, BLK), 1)).astype(F32).astype(BF16)
    sel = g_ref[...] >= 0.0
    pos = _dot(jnp.where(sel, 1.0, 0.0).astype(BF16), tri, 1, 0).astype(I32)
    slot_ref[...] = jnp.where(sel, pos + start_ref[...], -1)


def _onehot(code_ref, i, k, slot_ref, g_ref, hot_ref, gate_ref, n_exp):
    for q in range(PER):
        code = code_ref[i, k * PER + q]
        e = lax.rem(code, GRP)
        ids = lax.broadcasted_iota(I32, (GRP, BLK), 0) + (k * STEP + q * GRP)
        at = pl.ds(i * n_exp + e, 1)
        eq = slot_ref[at, :] == ids
        rows = slice(q * GRP, (q + 1) * GRP)
        hot_ref[rows, :] = jnp.where(eq, 1.0, 0.0).astype(BF16)
        gate_ref[rows, :] = jnp.where(eq, g_ref[at, :], 0.0)


def sort_kernel(meta_ref, code_ref, zero_ref, rel_ref, g_ref, start_ref, *rest, n_exp, n_blk, more):
    srcs = rest[:n_blk]
    rest = rest[more:]
    out_ref, slot_ref, x_ref, buf_ref, zbuf_ref, hot_ref, gate_ref, xsem, sem_ref, zsem = rest[n_blk:]
    hidden = x_ref.shape[2] // 2

    def zeros(q):
        return pltpu.make_async_copy(zbuf_ref, out_ref.at[pl.ds(pl.multiple_of(q * GRP, GRP), GRP), :], zsem.at[0])

    for k in range(n_blk):
        pltpu.make_async_copy(srcs[k], x_ref.at[k], xsem.at[k]).start()
    zbuf_ref[...] = jnp.zeros_like(zbuf_ref)
    for e in range(n_exp):
        lax.fori_loop(0, zero_ref[1, e], lambda q, c: (zeros(zero_ref[0, e] + q).start(), c)[1], 0)
    _slots(g_ref, start_ref, slot_ref)

    def drain(s, cnt):
        @pl.when(cnt == PER)
        def _():
            pltpu.make_async_copy(buf_ref.at[0], out_ref.at[pl.ds(0, STEP), :], sem_ref.at[s]).wait()

        @pl.when(cnt < PER)
        def _():
            def one(_, c):
                pltpu.make_async_copy(buf_ref.at[0, pl.ds(0, GRP), :], out_ref.at[pl.ds(0, GRP), :], sem_ref.at[s]).wait()
                return c

            lax.fori_loop(0, cnt, one, 0)

    def block(i, c):
        rel = rel_ref[i]
        n_grp = meta_ref[rel]
        pltpu.make_async_copy(srcs[0], x_ref.at[i], xsem.at[i]).wait()

        def step(k, c):
            s, old, newer = c
            _onehot(code_ref, rel, k, slot_ref, g_ref, hot_ref, gate_ref, n_exp)
            gcol = jnp.sum(gate_ref[...], axis=1, keepdims=True)
            hot = hot_ref[...]
            drain(s, old)
            buf_ref[s, :, :hidden] = _dot(hot, x_ref[i, :, :hidden], 1, 0).astype(BF16)
            buf_ref[s, :, hidden:] = (gcol * _dot(hot, x_ref[i, :, hidden:], 1, 0)).astype(BF16)
            cnt = jnp.minimum(n_grp - k * PER, PER)

            def send(q, c):
                code = code_ref[rel, k * PER + q]
                dst = pl.multiple_of(code - lax.rem(code, GRP), GRP)
                pltpu.make_async_copy(buf_ref.at[s, pl.ds(pl.multiple_of(q * GRP, GRP), GRP), :], out_ref.at[pl.ds(dst, GRP), :], sem_ref.at[s]).start()
                return c

            @pl.when(cnt == PER)
            def _():
                for q in range(PER):
                    send(q, 0)

            @pl.when(cnt < PER)
            def _():
                lax.fori_loop(0, cnt, send, 0)

            return 1 - s, newer, cnt

        return lax.fori_loop(0, (n_grp + PER - 1) // PER, step, c)

    s, old, newer = lax.fori_loop(0, n_blk, block, (jnp.int32(0), jnp.int32(0), jnp.int32(0)))
    drain(s, old)
    drain(1 - s, newer)
    for e in range(n_exp):
        lax.fori_loop(0, zero_ref[1, e], lambda q, c: (zeros(0).wait(), c)[1], 0)


def sort_rows(meta, code, zero, gates, start, blk, rels, rows, n_exp, into=None):
    blocks = [blk[k] for k in rels]
    n_blk = len(blocks)
    more = [] if into is None else [into]
    width = blocks[0].shape[1]
    smem = pl.BlockSpec(memory_space=pltpu.SMEM)
    vmem = pl.BlockSpec(memory_space=pltpu.VMEM)
    hbm = pl.BlockSpec(memory_space=pl.ANY)
    return pl.pallas_call(
        functools.partial(sort_kernel, n_exp=n_exp, n_blk=n_blk, more=len(more)),
        out_shape=jax.ShapeDtypeStruct((rows, width), BF16),
        in_specs=[smem] * 4 + [vmem] * 2 + [hbm] * (n_blk + len(more)),
        input_output_aliases={6 + n_blk: 0} if more else {},
        out_specs=hbm,
        scratch_shapes=[
            pltpu.VMEM(gates.shape, I32),
            pltpu.VMEM((n_blk, BLK, width), BF16),
            pltpu.VMEM((2, STEP, width), BF16),
            pltpu.VMEM((GRP, width), BF16),
            pltpu.VMEM((STEP, BLK), BF16),
            pltpu.VMEM((STEP, BLK), F32),
            pltpu.SemaphoreType.DMA((n_blk,)),
            pltpu.SemaphoreType.DMA((2,)),
            pltpu.SemaphoreType.DMA((1,)),
        ],
        cost_estimate=pl.CostEstimate(flops=1_500_000_000 * n_blk, bytes_accessed=3_000_000 * n_blk, transcendentals=0),
    )(meta, code, zero, jnp.array(rels, I32), gates, start, *blocks, *more)


def _units(first, n, src_ref, buf_ref, sem, slot, op):
    for j in range(MOST):

        @pl.when(j < n)
        def _():
            row = pl.multiple_of((first + j) * UNIT, UNIT)
            op(pltpu.make_async_copy(src_ref.at[pl.ds(row, UNIT), :], buf_ref.at[slot, pl.ds(j * UNIT, UNIT), :], sem.at[slot]))


def _start(c):
    c.start()


def _wait(c):
    c.wait()


def _piece(n, k):
    cuts = (n + MOST - 1) // MOST
    low = n // cuts
    extra = n - low * cuts
    return k * low + jnp.minimum(k, extra), low + jnp.where(k < extra, 1, 0), cuts


def _next(t_ref, e, k, cuts, n_exp):
    here = _piece(t_ref[1, e], jnp.minimum(k + 1, cuts - 1))[1]
    there = jnp.where(e + 1 < n_exp, _piece(t_ref[1, jnp.minimum(e + 1, n_exp - 1)], 0)[1], 0)
    return jnp.where(k + 1 < cuts, here, there)


def _hidden(u, d, w1_ref, w3_ref, w2_ref, j, w):
    h1 = _dot(u, w1_ref[0, :, j : j + w], 1, 0)
    h3 = _dot(u, w3_ref[0, :, j : j + w], 1, 0)
    da = _dot(d, w2_ref[0, j : j + w, :], 1, 1)
    sig = jax.nn.sigmoid(h1)
    silu = h1 * sig
    act = (silu * h3).astype(BF16)
    dh1 = (da * h3 * sig * (1.0 + h1 * (1.0 - sig))).astype(BF16)
    dh3 = (da * silu).astype(BF16)
    return act, dh1, dh3


def own_kernel(t_ref, ud_ref, w1_ref, w3_ref, w2_ref, o_ref, sv_ref, in_ref, ob_ref, sb_ref, cnt_ref, isem, osem, ssem, *, n_exp, hidden, inner):
    e = pl.program_id(0)

    def put(g, n, s, op):
        for j in range(MOST):

            @pl.when(j < n)
            def _():
                rows = pl.ds(pl.multiple_of((g + j) * UNIT, UNIT), UNIT)
                op(pltpu.make_async_copy(ob_ref.at[s, pl.ds(j * UNIT, UNIT), :], o_ref.at[rows, :], osem.at[s]))
                op(pltpu.make_async_copy(sb_ref.at[s, pl.ds(j * UNIT, UNIT), :], sv_ref.at[rows, :], ssem.at[s]))

    @pl.when(e == 0)
    def _():
        cnt_ref[0] = 0
        cnt_ref[1] = 0
        cnt_ref[2] = 0
        _units(0, _piece(t_ref[1, 0], 0)[1], ud_ref, in_ref, isem, 0, _start)

    def piece(k, c):
        off, n, cuts = _piece(t_ref[1, e], k)
        g = t_ref[0, e] + off
        s = lax.rem(cnt_ref[2], 2)
        cnt_ref[2] = cnt_ref[2] + 1
        _units(g, n, ud_ref, in_ref, isem, s, _wait)
        _units(g + n, _next(t_ref, e, k, cuts, n_exp), ud_ref, in_ref, isem, 1 - s, _start)
        put(0, cnt_ref[s], s, _wait)
        cnt_ref[s] = n
        for size in range(1, MOST + 1):

            @pl.when(n == size)
            def _():
                r = size * UNIT
                for j in range(0, inner, 256):
                    act, dh1, dh3 = _hidden(in_ref[s, :r, :hidden], in_ref[s, :r, hidden:], w1_ref, w3_ref, w2_ref, j, 256)
                    sb_ref[s, :r, j : j + 256] = act
                    sb_ref[s, :r, inner + j : inner + j + 256] = dh1
                    sb_ref[s, :r, 2 * inner + j : 2 * inner + j + 256] = dh3
                ob_ref[s, :r, :hidden] = _dot(sb_ref[s, :r, :inner], w2_ref[0], 1, 0).astype(BF16)
                ob_ref[s, :r, hidden:] = (_dot(sb_ref[s, :r, inner : 2 * inner], w1_ref[0], 1, 1) + _dot(sb_ref[s, :r, 2 * inner :], w3_ref[0], 1, 1)).astype(BF16)

        put(g, n, s, _start)
        return c

    lax.fori_loop(0, (t_ref[1, e] + MOST - 1) // MOST, piece, 0)

    @pl.when(e == n_exp - 1)
    def _():
        for s in range(2):
            put(0, cnt_ref[s], s, _wait)


def own_rows(table, ud, w1, w3, w2):
    n_exp, hidden, inner = w1.shape
    n_row, width = ud.shape
    wspec = lambda a, b: pl.BlockSpec((1, a, b), lambda e, t: (e, 0, 0))
    hbm = pl.BlockSpec(memory_space=pl.ANY)
    spec = pltpu.PrefetchScalarGridSpec(
        num_scalar_prefetch=1,
        grid=(n_exp,),
        in_specs=[hbm, wspec(hidden, inner), wspec(hidden, inner), wspec(inner, hidden)],
        out_specs=[hbm, hbm],
        scratch_shapes=[
            pltpu.VMEM((2, MOST * UNIT, width), BF16),
            pltpu.VMEM((2, MOST * UNIT, width), BF16),
            pltpu.VMEM((2, MOST * UNIT, 3 * inner), BF16),
            pltpu.SMEM((3,), I32),
            pltpu.SemaphoreType.DMA((2,)),
            pltpu.SemaphoreType.DMA((2,)),
            pltpu.SemaphoreType.DMA((2,)),
        ],
    )
    return pl.pallas_call(
        functools.partial(own_kernel, n_exp=n_exp, hidden=hidden, inner=inner),
        out_shape=[jax.ShapeDtypeStruct((n_row, width), BF16), jax.ShapeDtypeStruct((n_row, 3 * inner), BF16)],
        grid_spec=spec,
        name='own_rows',
        cost_estimate=pl.CostEstimate(flops=30_000_000_000, bytes_accessed=60_000_000, transcendentals=2_000_000),
    )(table, ud, w1, w3, w2)


def grads_kernel(ta_ref, tb_ref, uo_ref, sv_ref, ud_ref, w1_ref, w3_ref, w2_ref, g1_ref, g3_ref, g2_ref, oin_ref, sin_ref, in_ref, act_ref, dh_ref, cnt_ref, osem, ssem, isem, *, n_exp, hidden, inner):
    e = pl.program_id(0)

    @pl.when(e == 0)
    def _():
        cnt_ref[0] = 0
        cnt_ref[1] = 0
        n = _piece(ta_ref[1, 0], 0)[1]
        _units(0, n, uo_ref, oin_ref, osem, 0, _start)
        _units(0, n, sv_ref, sin_ref, ssem, 0, _start)
        _units(0, _piece(tb_ref[1, 0], 0)[1], ud_ref, in_ref, isem, 0, _start)

    mc = 256

    def outer(x_ref, s, r, act, dh1, dh3, fresh):
        def put(ref, m, v):
            ref[0, m : m + mc, :] = v if fresh else ref[0, m : m + mc, :] + v

        for m in range(0, hidden, mc):
            u = x_ref[s, :r, m : m + mc]
            put(g1_ref, m, _dot(u, dh1, 0, 0))
            put(g3_ref, m, _dot(u, dh3, 0, 0))
        d = x_ref[s, :r, hidden:]
        for m in range(0, inner, mc):
            put(g2_ref, m, _dot(act[:, m : m + mc], d, 0, 0))

    def own_piece(k, c):
        off, n, cuts = _piece(ta_ref[1, e], k)
        g = ta_ref[0, e] + off
        s = lax.rem(cnt_ref[0], 2)
        cnt_ref[0] = cnt_ref[0] + 1
        _units(g, n, uo_ref, oin_ref, osem, s, _wait)
        _units(g, n, sv_ref, sin_ref, ssem, s, _wait)
        m = _next(ta_ref, e, k, cuts, n_exp)
        _units(g + n, m, uo_ref, oin_ref, osem, 1 - s, _start)
        _units(g + n, m, sv_ref, sin_ref, ssem, 1 - s, _start)
        for size, fresh in [(v, True) for v in range(1, MOST + 1)] + [(v, False) for v in range(2, MOST + 1)]:

            @pl.when(jnp.logical_and(n == size, (k == 0) == fresh))
            def _():
                r = size * UNIT
                outer(oin_ref, s, r, sin_ref[s, :r, :inner], sin_ref[s, :r, inner : 2 * inner], sin_ref[s, :r, 2 * inner :], fresh)

        return c

    lax.fori_loop(0, (ta_ref[1, e] + MOST - 1) // MOST, own_piece, 0)

    def piece(k, c):
        off, n, cuts = _piece(tb_ref[1, e], k)
        g = tb_ref[0, e] + off
        s = lax.rem(cnt_ref[1], 2)
        cnt_ref[1] = cnt_ref[1] + 1
        _units(g, n, ud_ref, in_ref, isem, s, _wait)
        _units(g + n, _next(tb_ref, e, k, cuts, n_exp), ud_ref, in_ref, isem, 1 - s, _start)
        for size in range(1, MOST + 1):

            @pl.when(n == size)
            def _():
                r = size * UNIT
                for j in range(0, inner, mc):
                    act, dh1, dh3 = _hidden(in_ref[s, :r, :hidden], in_ref[s, :r, hidden:], w1_ref, w3_ref, w2_ref, j, mc)
                    act_ref[:r, j : j + mc] = act
                    dh_ref[:r, j : j + mc] = dh1
                    dh_ref[:r, inner + j : inner + j + mc] = dh3
                outer(in_ref, s, r, act_ref[:r, :], dh_ref[:r, :inner], dh_ref[:r, inner:], False)

        return c

    lax.fori_loop(0, (tb_ref[1, e] + MOST - 1) // MOST, piece, 0)


def weight_grads(ta, tb, uo, sv, ud, w1, w3, w2):
    n_exp, hidden, inner = w1.shape
    width = ud.shape[1]
    wspec = lambda a, b: pl.BlockSpec((1, a, b), lambda e, t, s: (e, 0, 0))
    hbm = pl.BlockSpec(memory_space=pl.ANY)
    most = MOST * UNIT
    spec = pltpu.PrefetchScalarGridSpec(
        num_scalar_prefetch=2,
        grid=(n_exp,),
        in_specs=[hbm, hbm, hbm, wspec(hidden, inner), wspec(hidden, inner), wspec(inner, hidden)],
        out_specs=[wspec(hidden, inner), wspec(hidden, inner), wspec(inner, hidden)],
        scratch_shapes=[
            pltpu.VMEM((2, most, width), BF16),
            pltpu.VMEM((2, most, 3 * inner), BF16),
            pltpu.VMEM((2, most, width), BF16),
            pltpu.VMEM((most, inner), BF16),
            pltpu.VMEM((most, 2 * inner), BF16),
            pltpu.SMEM((2,), I32),
            pltpu.SemaphoreType.DMA((2,)),
            pltpu.SemaphoreType.DMA((2,)),
            pltpu.SemaphoreType.DMA((2,)),
        ],
    )
    return pl.pallas_call(
        functools.partial(grads_kernel, n_exp=n_exp, hidden=hidden, inner=inner),
        out_shape=[jax.ShapeDtypeStruct(w.shape, F32) for w in (w1, w3, w2)],
        grid_spec=spec,
        name='weight_grads',
        cost_estimate=pl.CostEstimate(flops=90_000_000_000, bytes_accessed=150_000_000, transcendentals=4_000_000),
    )(ta, tb, uo, sv, ud, w1, w3, w2)


def combine_kernel(meta_ref, code_ref, g_ref, start_ref, r_ref_a, r_ref_b, o_ref, *rest, n_exp, hidden, which, more):
    if more:
        add_ref, keep_ref, go_ref, dg_ref, p_ref, slot_ref, buf_ref, hot_ref, gate_ref, sem_ref = rest
    else:
        p_ref, dg_ref, slot_ref, buf_ref, hot_ref, gate_ref, sem_ref = rest
    i = pl.program_id(0)

    def rel(k):
        return which[0] + k * (which[1] - which[0])

    def pull(k, s):
        def one(q, c):
            code = code_ref[rel(k), q]
            src = pl.multiple_of(code - lax.rem(code, GRP), GRP)
            pltpu.make_async_copy(o_ref.at[pl.ds(src, GRP), :], buf_ref.at[s, pl.ds(pl.multiple_of(q * GRP, GRP), GRP), :], sem_ref.at[s]).start()
            return c

        lax.fori_loop(0, meta_ref[rel(k)], one, 0)

    @pl.when(i == 0)
    def _():
        pull(0, 0)
        pull(1, 1)
        _slots(g_ref, start_ref, slot_ref)

    n_grp = meta_ref[rel(i)]
    n_step = (n_grp + PER - 1) // PER

    def blank(q, c):
        buf_ref[i, pl.ds(pl.multiple_of(q * GRP, GRP), GRP), :] = jnp.zeros((GRP, buf_ref.shape[2]), BF16)
        return c

    lax.fori_loop(n_grp, n_step * PER, blank, 0)
    if more:
        p_ref[...] = add_ref[...]
    else:
        p_ref[...] = jnp.zeros_like(p_ref)
    dg_ref[...] = jnp.zeros_like(dg_ref)

    def whole(q, c):
        pltpu.make_async_copy(o_ref.at[pl.ds(0, STEP), :], buf_ref.at[0, pl.ds(0, STEP), :], sem_ref.at[i]).wait()
        return c

    def single(q, c):
        pltpu.make_async_copy(o_ref.at[pl.ds(0, GRP), :], buf_ref.at[0, pl.ds(0, GRP), :], sem_ref.at[i]).wait()
        return c

    lax.fori_loop(0, n_grp // PER, whole, 0)
    lax.fori_loop(0, lax.rem(n_grp, PER), single, 0)

    def step(k, c):
        rows = pl.ds(pl.multiple_of(k * STEP, STEP), STEP)
        o = buf_ref[i, rows, :hidden]
        rg = buf_ref[i, rows, hidden:]
        prod = _dot(o, jnp.where(i == 0, r_ref_a[...], r_ref_b[...]), 1, 1)
        _onehot(code_ref, rel(i), k, slot_ref, g_ref, hot_ref, gate_ref, n_exp)
        hot = hot_ref[...]
        prod = jnp.where(hot.astype(F32) > 0.5, prod, 0.0)
        for q in range(PER):
            e = lax.rem(code_ref[rel(i), k * PER + q], GRP)
            dg_ref[0, pl.ds(e, 1), :] += jnp.sum(prod[q * GRP : (q + 1) * GRP, :], axis=0, keepdims=True)
        gsel = gate_ref[...]
        g_hi = gsel.astype(BF16)
        rest = gsel - g_hi.astype(F32)
        g_mid = rest.astype(BF16)
        g_lo = (rest - g_mid.astype(F32)).astype(BF16)
        p_ref[:, :hidden] += _dot(g_hi, o, 0, 0) + (_dot(g_mid, o, 0, 0) + _dot(g_lo, o, 0, 0))
        p_ref[:, hidden:] += _dot(hot, rg, 0, 0)
        return c

    lax.fori_loop(0, n_step, step, 0)
    if more:

        @pl.when(i == 0)
        def _():
            keep_ref[...] = p_ref[...]

        @pl.when(i == 1)
        def _():
            go_ref[...] = p_ref[...]


def combine(meta, code, gates, start, blocks, o_rows, which, n_exp, add=None):
    width = o_rows.shape[1]
    hidden = width // 2
    half = pl.BlockSpec((BLK, hidden), lambda i, m, s: (0, 1))
    block = pl.BlockSpec((BLK, width), lambda i, m, s: (i, 0))
    more = [] if add is None else [add]
    whole = pl.BlockSpec(gates.shape, lambda i, m, s: (0, 0))
    fixed = pl.BlockSpec((BLK, width), lambda i, m, s: (0, 0))
    spec = pltpu.PrefetchScalarGridSpec(
        num_scalar_prefetch=2,
        grid=(2,),
        in_specs=[
            whole,
            whole,
            half,
            half,
            pl.BlockSpec(memory_space=pl.ANY),
            *([block] * len(more)),
        ],
        out_specs=([fixed] * 2 if more else [block]) + [pl.BlockSpec((1, n_exp, BLK), lambda i, m, s: (i, 0, 0))],
        scratch_shapes=[
            *([pltpu.VMEM((BLK, width), F32)] * len(more)),
            pltpu.VMEM(gates.shape, I32),
            pltpu.VMEM((2, BLK * n_exp, width), BF16),
            pltpu.VMEM((STEP, BLK), BF16),
            pltpu.VMEM((STEP, BLK), F32),
            pltpu.SemaphoreType.DMA((2,)),
        ],
    )
    return pl.pallas_call(
        functools.partial(combine_kernel, n_exp=n_exp, hidden=hidden, which=which, more=bool(more)),
        out_shape=([jax.ShapeDtypeStruct((BLK, width), F32)] * 2 if more else [jax.ShapeDtypeStruct((2 * BLK, width), F32)]) + [jax.ShapeDtypeStruct((2, n_exp, BLK), F32)],
        grid_spec=spec,
        name='combine',
        cost_estimate=pl.CostEstimate(flops=8_000_000_000, bytes_accessed=20_000_000, transcendentals=0),
    )(meta, code, gates, start, blocks[which[0]], blocks[which[1]], o_rows, *more)


def routing_tables(cnt, n_own):
    n_blk, n_exp = cnt.shape
    pad = (cnt + GRP - 1) // GRP * GRP
    before_e = (jnp.arange(n_exp)[:, None] < jnp.arange(n_exp)[None, :]).astype(I32)
    blk = jnp.arange(n_blk)
    same = (blk[:, None] < n_own) == (blk[None, :] < n_own)
    before_b = ((blk[:, None] < blk[None, :]) & same).astype(I32)
    blk_start = jnp.sum(pad[:, :, None] * before_e[None], axis=1)
    blk_end = blk_start + pad
    in_exp = jnp.sum(pad[:, None, :] * before_b[:, :, None], axis=0)

    def part(p):
        total = jnp.sum(p, axis=0)
        units = jnp.maximum((total + UNIT - 1) // UNIT, 1)
        first = jnp.sum(units[:, None] * before_e, axis=0)
        zero = jnp.stack([(first * UNIT + total) // GRP, (units * UNIT - total) // GRP])
        return jnp.stack([first, units]).astype(I32), zero.astype(I32), first * UNIT

    ta, za, base_a = part(pad[:n_own])
    tb, zb, base_b = part(pad[n_own:])
    base = jnp.where(blk[:, None] < n_own, base_a[None], base_b[None])
    q = jnp.arange(BLK * n_exp // GRP, dtype=I32) * GRP
    inside = (q[None, :, None] >= blk_start[:, None, :]) & (q[None, :, None] < blk_end[:, None, :])
    place = base + in_exp - blk_start + jnp.arange(n_exp, dtype=I32)[None]
    code = jnp.sum(jnp.where(inside, place[:, None, :] + q[None, :, None], 0), axis=2)
    start = jnp.broadcast_to(blk_start.reshape(n_blk * n_exp, 1), (n_blk * n_exp, BLK)).astype(I32)
    return (jnp.sum(pad, axis=1) // GRP).astype(I32), start, code.astype(I32), ta, za, tb, zb


def solution(mesh):
    ep_size = mesh.shape['ep']
    dp_size = mesh.shape['dp']
    n_dev = ep_size * dp_size
    all_axes = ('dp', 'ep')

    def swap(v, mask):
        return lax.ppermute(v, all_axes, [(d, d ^ mask) for d in range(n_dev)])

    def layer(tokens, w_router, w_gate, w_up, w_down, top_ids, r_proj):
        n_local, hidden = tokens.shape
        local_exp = w_gate.shape[0]
        xr = jnp.concatenate([tokens, r_proj], axis=1)
        blk = {0: xr}
        own_gates, gates, *got = first_stage(tokens, w_router.T, top_ids.T, xr, n_dev, ep_size)
        blk.update(zip((1, 2, 4, 8, 3, 5, 9), got))
        for dst, src, mask in ((6, 4, 2), (12, 8, 4), (10, 2, 8)):
            blk[dst] = swap(blk[src], mask)
        cnt = jnp.sum((gates >= 0).astype(I32), axis=2)
        gates = gates.reshape(n_dev * local_exp, n_local)
        meta, start, code, ta, za, tb, zb = routing_tables(cnt, ep_size)
        own_n = ep_size * n_local * local_exp + local_exp * UNIT
        oth_n = (n_dev - ep_size) * n_local * local_exp + local_exp * UNIT
        uo = sort_rows(meta, code, za, gates, start, blk, (0, 1, 2, 3), own_n, local_exp)
        o_rows, sv = own_rows(ta, uo, w_gate, w_up, w_down)
        o_rows, blk[6], blk[10], blk[12] = lax.optimization_barrier((o_rows, blk[6], blk[10], blk[12]))
        c0, c1 = 96, 176
        far = []
        for v, mask in ((blk[12][:c0], 2), (blk[10][c0:c1], 4), (blk[6][c1:], 8)):
            far.append(swap(v, mask))
        for k in (6, 10, 12):
            blk[k + 1] = swap(blk[k], 1)
        ud = sort_rows(meta, code, zb, gates, start, blk, (4, 5, 8, 9, 6, 10, 12), oth_n, local_exp)
        blk[14] = jnp.concatenate(far, axis=0)
        blk[15] = swap(blk[14], 1)
        p_send, dg_b = combine(meta, code, gates, start, blk, o_rows, (1, 3), local_exp)
        p_sib = swap(p_send, 1)
        ud = sort_rows(meta, code, jnp.zeros_like(zb), gates, start, blk, (7, 11, 13, 14, 15), oth_n, local_exp, ud)
        p_sib, ud = lax.optimization_barrier((p_sib, ud))
        p_keep, p_go, dg_a = combine(meta, code, gates, start, blk, o_rows, (0, 2), local_exp, p_sib)
        dg = jnp.stack([dg_a[0], dg_b[0], dg_a[1], dg_b[1]])
        dz_t, grad_router_t = router_backward(dg, own_gates, tokens, n_dev, ep_size)
        p_go, dz_t = lax.optimization_barrier((p_go, dz_t))
        p_far = swap(p_go, 2)
        g_gate, g_up, g_down = weight_grads(ta, tb, uo, sv, ud, w_gate, w_up, w_down)
        grad_router = grad_router_t.T
        y = tokens.astype(F32) + (p_keep[:, :hidden] + p_far[:, :hidden])
        dx = r_proj.astype(F32) + _dot(dz_t, w_router, 0, 1) + (p_keep[:, hidden:] + p_far[:, hidden:])
        return y, dx, g_gate, g_up, g_down, grad_router

    tok_spec = P(all_axes, None)
    exp_spec = P('ep', None, None)
    return jax.shard_map(layer, mesh=mesh, in_specs=(tok_spec, P(), exp_spec, exp_spec, exp_spec, tok_spec, tok_spec), out_specs=(tok_spec, tok_spec, exp_spec, exp_spec, exp_spec, P()), check_vma=False)
```

```python
import functools

import jax
import jax.numpy as jnp
from jax import lax
from jax.experimental import pallas as pl
from jax.experimental.pallas import tpu as pltpu
from jax.sharding import PartitionSpec as P


F32 = jnp.float32
BF16 = jnp.bfloat16
I32 = jnp.int32
GRP = 16
UNIT = 128
MOST = 4
STEP = 256
BLK = 256
PER = STEP // GRP
MESH = pl.DeviceIdType.MESH


def _dot(a, b, ca, cb):
    return lax.dot_general(a, b, (((ca,), (cb,)), ((), ())), preferred_element_type=F32)


def _flip(v, mask):
    for k in range(2):
        if (mask >> k) & 1:
            v = v + (1 << k) * (1 - 2 * ((v // (1 << k)) % 2))
    return v


def _peers(dp, ep, ep_size, n_dev):
    return {r: (_flip(dp, r // ep_size), _flip(ep, r % ep_size)) for r in range(1, n_dev)}


def _greet(peers):
    barrier = pltpu.get_barrier_semaphore()
    for peer in peers.values():
        pl.semaphore_signal(barrier, inc=1, device_id=peer, device_id_type=MESH)
    pl.semaphore_wait(barrier, len(peers))


def first_kernel(x_ref, wr_ref, ids_ref, xr_ref, own_ref, out_ref, b1, b2, b4, b8, b3, b5, b9, ssem, rsem, bsend, brecv, fsend, frecv, *, n_dev, ep_size):
    dp, ep = lax.axis_index('dp'), lax.axis_index('ep')
    peers = _peers(dp, ep, ep_size, n_dev)
    local = out_ref.shape[1]
    _greet(peers)

    def copy(src, dst, s, r, k, mask):
        return pltpu.make_async_remote_copy(src_ref=src, dst_ref=dst, send_sem=s.at[k], recv_sem=r.at[k], device_id=peers[mask], device_id_type=MESH)

    half = xr_ref.shape[0] // 2
    part = [pl.ds(0, half), pl.ds(half, half)]
    direct = []
    for h in range(2):
        for k, (dst, mask) in enumerate(((b2, 2), (b4, 4), (b8, 8), (b1, 1))):
            direct.append(copy(xr_ref.at[part[h], :], dst.at[part[h], :], bsend, brecv, 4 * h + k, mask))
    for c in direct[:4]:
        c.start()
    z = _dot(wr_ref[...], x_ref[...], 1, 1)
    eid = lax.broadcasted_iota(I32, z.shape, 0)
    sel = eid == ids_ref[0:1, :]
    for j in range(1, ids_ref.shape[0]):
        sel = jnp.logical_or(sel, eid == ids_ref[j : j + 1, :])
    peak = jnp.max(jnp.where(sel, z, -3.0e38), axis=0, keepdims=True)
    ex = jnp.where(sel, jnp.exp(jnp.where(sel, z - peak, 0.0)), 0.0)
    gates = ex / jnp.sum(ex, axis=0, keepdims=True)
    marked = jnp.where(sel, gates, -1.0)
    for k in range(ep_size):
        own_ref[k] = marked[k * local : (k + 1) * local, :]
    out_ref[0] = own_ref[ep]
    direct[3].wait_recv()
    small = [copy(own_ref.at[peer[1]], out_ref.at[r], ssem, rsem, r, r) for r, peer in peers.items()]
    for c in small + direct[4:]:
        c.start()
    passed = []
    for h in range(2):
        for k, (src, dst) in enumerate(((b2, b3), (b4, b5), (b8, b9))):
            direct[4 * h + k].wait_recv()
            passed.append(copy(src.at[part[h], :], dst.at[part[h], :], fsend, frecv, 3 * h + k, 1))
            passed[-1].start()
    direct[7].wait_recv()
    for c in direct:
        c.wait_send()
    for c in passed + small:
        c.wait()


def first_stage(tokens, w_router, ids_t, xr, n_dev, ep_size):
    local = w_router.shape[0] // ep_size
    n_tok = tokens.shape[0]
    vmem = pl.BlockSpec(memory_space=pltpu.VMEM)
    hbm = pl.BlockSpec(memory_space=pl.ANY)
    dma = pltpu.SemaphoreType.DMA
    return pl.pallas_call(
        functools.partial(first_kernel, n_dev=n_dev, ep_size=ep_size),
        out_shape=[jax.ShapeDtypeStruct((ep_size, local, n_tok), F32), jax.ShapeDtypeStruct((n_dev, local, n_tok), F32)] + [jax.ShapeDtypeStruct(xr.shape, BF16)] * 7,
        in_specs=[vmem] * 3 + [hbm],
        out_specs=[vmem] * 2 + [hbm] * 7,
        scratch_shapes=[dma((n_dev,)), dma((n_dev,)), dma((8,)), dma((8,)), dma((6,)), dma((6,))],
        compiler_params=pltpu.CompilerParams(collective_id=0, has_side_effects=True),
        cost_estimate=pl.CostEstimate(flops=20_000_000_000, bytes_accessed=20_000_000, transcendentals=0),
        name='first_stage',
    )(tokens, w_router, ids_t, xr)


def router_kernel(dg_ref, g_ref, x_ref, dz_ref, out_ref, gr_ref, all_ref, part_ref, take_ref, sem_a, sem_b, sem_c, sem_d, sem_e, sem_f, *, n_dev, ep_size):
    dp, ep = lax.axis_index('dp'), lax.axis_index('ep')
    me = dp * ep_size + ep
    peers = _peers(dp, ep, ep_size, n_dev)
    all_ref[ep] = dg_ref[0]
    _greet(peers)
    copies = []
    for r in range(1, ep_size):
        copies.append(pltpu.make_async_remote_copy(src_ref=dg_ref.at[r], dst_ref=all_ref.at[ep], send_sem=sem_a.at[r], recv_sem=sem_b.at[r], device_id=peers[r], device_id_type=MESH))
        copies[-1].start()
    for c in copies:
        c.wait()
    g = jnp.maximum(jnp.concatenate([g_ref[k] for k in range(ep_size)], axis=0), 0.0)
    dg = jnp.concatenate([all_ref[k] for k in range(ep_size)], axis=0)
    dz = (g * (dg - jnp.sum(g * dg, axis=0, keepdims=True))).astype(BF16)
    dz_ref[...] = dz
    part = _dot(dz, x_ref[...], 1, 0)
    rows = part.shape[0] // n_dev
    for k in range(n_dev):
        part_ref[k] = part[k * rows : (k + 1) * rows, :]
    take_ref[me] = part_ref[me]
    copies = []
    for r, peer in peers.items():
        pid = peer[0] * ep_size + peer[1]
        copies.append(pltpu.make_async_remote_copy(src_ref=part_ref.at[pid], dst_ref=take_ref.at[me], send_sem=sem_c.at[r], recv_sem=sem_d.at[r], device_id=peer, device_id_type=MESH))
        copies[-1].start()
    for c in copies:
        c.wait()
    total = take_ref[0]
    for k in range(1, n_dev):
        total = total + take_ref[k]
    gr_ref[me] = total
    copies = []
    for r, peer in peers.items():
        copies.append(pltpu.make_async_remote_copy(src_ref=gr_ref.at[me], dst_ref=gr_ref.at[me], send_sem=sem_e.at[r], recv_sem=sem_f.at[r], device_id=peer, device_id_type=MESH))
        copies[-1].start()
    for c in copies:
        c.wait()
    out_ref[...] = jnp.concatenate([gr_ref[k] for k in range(n_dev)], axis=0)


def router_backward(dg, gates, tokens, n_dev, ep_size):
    n_exp = gates.shape[0] * gates.shape[1]
    n_tok, hidden = tokens.shape
    vmem = pl.BlockSpec(memory_space=pltpu.VMEM)
    rows = n_exp // n_dev
    dma = pltpu.SemaphoreType.DMA((n_dev,))
    return pl.pallas_call(
        functools.partial(router_kernel, n_dev=n_dev, ep_size=ep_size),
        out_shape=[jax.ShapeDtypeStruct((n_exp, n_tok), BF16), jax.ShapeDtypeStruct((n_exp, hidden), F32)],
        in_specs=[vmem] * 3,
        out_specs=[vmem] * 2,
        scratch_shapes=[
            pltpu.VMEM((n_dev, rows, hidden), F32),
            pltpu.VMEM((ep_size, n_exp // ep_size, n_tok), F32),
            pltpu.VMEM((n_dev, rows, hidden), F32),
            pltpu.VMEM((n_dev, rows, hidden), F32),
            *([dma] * 6),
        ],
        compiler_params=pltpu.CompilerParams(collective_id=1, has_side_effects=True),
        cost_estimate=pl.CostEstimate(flops=2_000_000_000, bytes_accessed=2_000_000, transcendentals=0),
        name='router_backward',
    )(dg, gates, tokens)


def _slots(g_ref, start_ref, slot_ref):
    tri = (lax.broadcasted_iota(I32, (BLK, BLK), 0) < lax.broadcasted_iota(I32, (BLK, BLK), 1)).astype(F32).astype(BF16)
    sel = g_ref[...] >= 0.0
    pos = _dot(jnp.where(sel, 1.0, 0.0).astype(BF16), tri, 1, 0).astype(I32)
    slot_ref[...] = jnp.where(sel, pos + start_ref[...], -1)


def _onehot(code_ref, i, k, slot_ref, g_ref, hot_ref, gate_ref, n_exp):
    for q in range(PER):
        code = code_ref[i, k * PER + q]
        e = lax.rem(code, GRP)
        ids = lax.broadcasted_iota(I32, (GRP, BLK), 0) + (k * STEP + q * GRP)
        at = pl.ds(i * n_exp + e, 1)
        eq = slot_ref[at, :] == ids
        rows = slice(q * GRP, (q + 1) * GRP)
        hot_ref[rows, :] = jnp.where(eq, 1.0, 0.0).astype(BF16)
        gate_ref[rows, :] = jnp.where(eq, g_ref[at, :], 0.0)


def sort_kernel(meta_ref, code_ref, zero_ref, rel_ref, g_ref, start_ref, *rest, n_exp, n_blk, more):
    srcs = rest[:n_blk]
    rest = rest[more:]
    out_ref, slot_ref, x_ref, buf_ref, zbuf_ref, hot_ref, gate_ref, xsem, sem_ref, zsem = rest[n_blk:]
    hidden = x_ref.shape[2] // 2

    def zeros(q):
        return pltpu.make_async_copy(zbuf_ref, out_ref.at[pl.ds(pl.multiple_of(q * GRP, GRP), GRP), :], zsem.at[0])

    for k in range(n_blk):
        pltpu.make_async_copy(srcs[k], x_ref.at[k], xsem.at[k]).start()
    zbuf_ref[...] = jnp.zeros_like(zbuf_ref)
    for e in range(n_exp):
        lax.fori_loop(0, zero_ref[1, e], lambda q, c: (zeros(zero_ref[0, e] + q).start(), c)[1], 0)
    _slots(g_ref, start_ref, slot_ref)

    def drain(s, cnt):
        @pl.when(cnt == PER)
        def _():
            pltpu.make_async_copy(buf_ref.at[0], out_ref.at[pl.ds(0, STEP), :], sem_ref.at[s]).wait()

        @pl.when(cnt < PER)
        def _():
            def one(_, c):
                pltpu.make_async_copy(buf_ref.at[0, pl.ds(0, GRP), :], out_ref.at[pl.ds(0, GRP), :], sem_ref.at[s]).wait()
                return c

            lax.fori_loop(0, cnt, one, 0)

    def block(i, c):
        rel = rel_ref[i]
        n_grp = meta_ref[rel]
        pltpu.make_async_copy(srcs[0], x_ref.at[i], xsem.at[i]).wait()

        def step(k, c):
            s, old, newer = c
            _onehot(code_ref, rel, k, slot_ref, g_ref, hot_ref, gate_ref, n_exp)
            gcol = jnp.sum(gate_ref[...], axis=1, keepdims=True)
            hot = hot_ref[...]
            drain(s, old)
            buf_ref[s, :, :hidden] = _dot(hot, x_ref[i, :, :hidden], 1, 0).astype(BF16)
            buf_ref[s, :, hidden:] = (gcol * _dot(hot, x_ref[i, :, hidden:], 1, 0)).astype(BF16)
            cnt = jnp.minimum(n_grp - k * PER, PER)

            def send(q, c):
                code = code_ref[rel, k * PER + q]
                dst = pl.multiple_of(code - lax.rem(code, GRP), GRP)
                pltpu.make_async_copy(buf_ref.at[s, pl.ds(pl.multiple_of(q * GRP, GRP), GRP), :], out_ref.at[pl.ds(dst, GRP), :], sem_ref.at[s]).start()
                return c

            @pl.when(cnt == PER)
            def _():
                for q in range(PER):
                    send(q, 0)

            @pl.when(cnt < PER)
            def _():
                lax.fori_loop(0, cnt, send, 0)

            return 1 - s, newer, cnt

        return lax.fori_loop(0, (n_grp + PER - 1) // PER, step, c)

    s, old, newer = lax.fori_loop(0, n_blk, block, (jnp.int32(0), jnp.int32(0), jnp.int32(0)))
    drain(s, old)
    drain(1 - s, newer)
    for e in range(n_exp):
        lax.fori_loop(0, zero_ref[1, e], lambda q, c: (zeros(0).wait(), c)[1], 0)


def sort_rows(meta, code, zero, gates, start, blk, rels, rows, n_exp, into=None):
    blocks = [blk[k] for k in rels]
    n_blk = len(blocks)
    more = [] if into is None else [into]
    width = blocks[0].shape[1]
    smem = pl.BlockSpec(memory_space=pltpu.SMEM)
    vmem = pl.BlockSpec(memory_space=pltpu.VMEM)
    hbm = pl.BlockSpec(memory_space=pl.ANY)
    return pl.pallas_call(
        functools.partial(sort_kernel, n_exp=n_exp, n_blk=n_blk, more=len(more)),
        out_shape=jax.ShapeDtypeStruct((rows, width), BF16),
        in_specs=[smem] * 4 + [vmem] * 2 + [hbm] * (n_blk + len(more)),
        input_output_aliases={6 + n_blk: 0} if more else {},
        out_specs=hbm,
        scratch_shapes=[
            pltpu.VMEM(gates.shape, I32),
            pltpu.VMEM((n_blk, BLK, width), BF16),
            pltpu.VMEM((2, STEP, width), BF16),
            pltpu.VMEM((GRP, width), BF16),
            pltpu.VMEM((STEP, BLK), BF16),
            pltpu.VMEM((STEP, BLK), F32),
            pltpu.SemaphoreType.DMA((n_blk,)),
            pltpu.SemaphoreType.DMA((2,)),
            pltpu.SemaphoreType.DMA((1,)),
        ],
        cost_estimate=pl.CostEstimate(flops=1_500_000_000 * n_blk, bytes_accessed=3_000_000 * n_blk, transcendentals=0),
    )(meta, code, zero, jnp.array(rels, I32), gates, start, *blocks, *more)


def _units(first, n, src_ref, buf_ref, sem, slot, op):
    for j in range(MOST):

        @pl.when(j < n)
        def _():
            row = pl.multiple_of((first + j) * UNIT, UNIT)
            op(pltpu.make_async_copy(src_ref.at[pl.ds(row, UNIT), :], buf_ref.at[slot, pl.ds(j * UNIT, UNIT), :], sem.at[slot]))


def _start(c):
    c.start()


def _wait(c):
    c.wait()


def _piece(n, k):
    cuts = (n + MOST - 1) // MOST
    low = n // cuts
    extra = n - low * cuts
    return k * low + jnp.minimum(k, extra), low + jnp.where(k < extra, 1, 0), cuts


def _next(t_ref, e, k, cuts, n_exp):
    here = _piece(t_ref[1, e], jnp.minimum(k + 1, cuts - 1))[1]
    there = jnp.where(e + 1 < n_exp, _piece(t_ref[1, jnp.minimum(e + 1, n_exp - 1)], 0)[1], 0)
    return jnp.where(k + 1 < cuts, here, there)


def _hidden(u, d, w1_ref, w3_ref, w2_ref, j, w):
    h1 = _dot(u, w1_ref[0, :, j : j + w], 1, 0)
    h3 = _dot(u, w3_ref[0, :, j : j + w], 1, 0)
    da = _dot(d, w2_ref[0, j : j + w, :], 1, 1)
    sig = jax.nn.sigmoid(h1)
    silu = h1 * sig
    act = (silu * h3).astype(BF16)
    dh1 = (da * h3 * sig * (1.0 + h1 * (1.0 - sig))).astype(BF16)
    dh3 = (da * silu).astype(BF16)
    return act, dh1, dh3


def own_kernel(t_ref, ud_ref, w1_ref, w3_ref, w2_ref, o_ref, sv_ref, in_ref, ob_ref, sb_ref, cnt_ref, isem, osem, ssem, *, n_exp, hidden, inner):
    e = pl.program_id(0)

    def put(g, n, s, op):
        for j in range(MOST):

            @pl.when(j < n)
            def _():
                rows = pl.ds(pl.multiple_of((g + j) * UNIT, UNIT), UNIT)
                op(pltpu.make_async_copy(ob_ref.at[s, pl.ds(j * UNIT, UNIT), :], o_ref.at[rows, :], osem.at[s]))
                op(pltpu.make_async_copy(sb_ref.at[s, pl.ds(j * UNIT, UNIT), :], sv_ref.at[rows, :], ssem.at[s]))

    @pl.when(e == 0)
    def _():
        cnt_ref[0] = 0
        cnt_ref[1] = 0
        cnt_ref[2] = 0
        _units(0, _piece(t_ref[1, 0], 0)[1], ud_ref, in_ref, isem, 0, _start)

    def piece(k, c):
        off, n, cuts = _piece(t_ref[1, e], k)
        g = t_ref[0, e] + off
        s = lax.rem(cnt_ref[2], 2)
        cnt_ref[2] = cnt_ref[2] + 1
        _units(g, n, ud_ref, in_ref, isem, s, _wait)
        _units(g + n, _next(t_ref, e, k, cuts, n_exp), ud_ref, in_ref, isem, 1 - s, _start)
        put(0, cnt_ref[s], s, _wait)
        cnt_ref[s] = n
        for size in range(1, MOST + 1):

            @pl.when(n == size)
            def _():
                r = size * UNIT
                for j in range(0, inner, 256):
                    act, dh1, dh3 = _hidden(in_ref[s, :r, :hidden], in_ref[s, :r, hidden:], w1_ref, w3_ref, w2_ref, j, 256)
                    sb_ref[s, :r, j : j + 256] = act
                    sb_ref[s, :r, inner + j : inner + j + 256] = dh1
                    sb_ref[s, :r, 2 * inner + j : 2 * inner + j + 256] = dh3
                ob_ref[s, :r, :hidden] = _dot(sb_ref[s, :r, :inner], w2_ref[0], 1, 0).astype(BF16)
                ob_ref[s, :r, hidden:] = (_dot(sb_ref[s, :r, inner : 2 * inner], w1_ref[0], 1, 1) + _dot(sb_ref[s, :r, 2 * inner :], w3_ref[0], 1, 1)).astype(BF16)

        put(g, n, s, _start)
        return c

    lax.fori_loop(0, (t_ref[1, e] + MOST - 1) // MOST, piece, 0)

    @pl.when(e == n_exp - 1)
    def _():
        for s in range(2):
            put(0, cnt_ref[s], s, _wait)


def own_rows(table, ud, w1, w3, w2):
    n_exp, hidden, inner = w1.shape
    n_row, width = ud.shape
    wspec = lambda a, b: pl.BlockSpec((1, a, b), lambda e, t: (e, 0, 0))
    hbm = pl.BlockSpec(memory_space=pl.ANY)
    spec = pltpu.PrefetchScalarGridSpec(
        num_scalar_prefetch=1,
        grid=(n_exp,),
        in_specs=[hbm, wspec(hidden, inner), wspec(hidden, inner), wspec(inner, hidden)],
        out_specs=[hbm, hbm],
        scratch_shapes=[
            pltpu.VMEM((2, MOST * UNIT, width), BF16),
            pltpu.VMEM((2, MOST * UNIT, width), BF16),
            pltpu.VMEM((2, MOST * UNIT, 3 * inner), BF16),
            pltpu.SMEM((3,), I32),
            pltpu.SemaphoreType.DMA((2,)),
            pltpu.SemaphoreType.DMA((2,)),
            pltpu.SemaphoreType.DMA((2,)),
        ],
    )
    return pl.pallas_call(
        functools.partial(own_kernel, n_exp=n_exp, hidden=hidden, inner=inner),
        out_shape=[jax.ShapeDtypeStruct((n_row, width), BF16), jax.ShapeDtypeStruct((n_row, 3 * inner), BF16)],
        grid_spec=spec,
        name='own_rows',
        cost_estimate=pl.CostEstimate(flops=30_000_000_000, bytes_accessed=60_000_000, transcendentals=2_000_000),
    )(table, ud, w1, w3, w2)


def grads_kernel(ta_ref, tb_ref, uo_ref, sv_ref, ud_ref, w1_ref, w3_ref, w2_ref, g1_ref, g3_ref, g2_ref, oin_ref, sin_ref, in_ref, act_ref, dh_ref, cnt_ref, osem, ssem, isem, *, n_exp, hidden, inner):
    e = pl.program_id(0)

    @pl.when(e == 0)
    def _():
        cnt_ref[0] = 0
        cnt_ref[1] = 0
        n = _piece(ta_ref[1, 0], 0)[1]
        _units(0, n, uo_ref, oin_ref, osem, 0, _start)
        _units(0, n, sv_ref, sin_ref, ssem, 0, _start)
        _units(0, _piece(tb_ref[1, 0], 0)[1], ud_ref, in_ref, isem, 0, _start)

    mc = 256

    def outer(x_ref, s, r, act, dh1, dh3, fresh):
        def put(ref, m, v):
            ref[0, m : m + mc, :] = v if fresh else ref[0, m : m + mc, :] + v

        for m in range(0, hidden, mc):
            u = x_ref[s, :r, m : m + mc]
            put(g1_ref, m, _dot(u, dh1, 0, 0))
            put(g3_ref, m, _dot(u, dh3, 0, 0))
        d = x_ref[s, :r, hidden:]
        for m in range(0, inner, mc):
            put(g2_ref, m, _dot(act[:, m : m + mc], d, 0, 0))

    def own_piece(k, c):
        off, n, cuts = _piece(ta_ref[1, e], k)
        g = ta_ref[0, e] + off
        s = lax.rem(cnt_ref[0], 2)
        cnt_ref[0] = cnt_ref[0] + 1
        _units(g, n, uo_ref, oin_ref, osem, s, _wait)
        _units(g, n, sv_ref, sin_ref, ssem, s, _wait)
        m = _next(ta_ref, e, k, cuts, n_exp)
        _units(g + n, m, uo_ref, oin_ref, osem, 1 - s, _start)
        _units(g + n, m, sv_ref, sin_ref, ssem, 1 - s, _start)
        for size, fresh in [(v, True) for v in range(1, MOST + 1)] + [(v, False) for v in range(2, MOST + 1)]:

            @pl.when(jnp.logical_and(n == size, (k == 0) == fresh))
            def _():
                r = size * UNIT
                outer(oin_ref, s, r, sin_ref[s, :r, :inner], sin_ref[s, :r, inner : 2 * inner], sin_ref[s, :r, 2 * inner :], fresh)

        return c

    lax.fori_loop(0, (ta_ref[1, e] + MOST - 1) // MOST, own_piece, 0)

    def piece(k, c):
        off, n, cuts = _piece(tb_ref[1, e], k)
        g = tb_ref[0, e] + off
        s = lax.rem(cnt_ref[1], 2)
        cnt_ref[1] = cnt_ref[1] + 1
        _units(g, n, ud_ref, in_ref, isem, s, _wait)
        _units(g + n, _next(tb_ref, e, k, cuts, n_exp), ud_ref, in_ref, isem, 1 - s, _start)
        for size in range(1, MOST + 1):

            @pl.when(n == size)
            def _():
                r = size * UNIT
                for j in range(0, inner, mc):
                    act, dh1, dh3 = _hidden(in_ref[s, :r, :hidden], in_ref[s, :r, hidden:], w1_ref, w3_ref, w2_ref, j, mc)
                    act_ref[:r, j : j + mc] = act
                    dh_ref[:r, j : j + mc] = dh1
                    dh_ref[:r, inner + j : inner + j + mc] = dh3
                outer(in_ref, s, r, act_ref[:r, :], dh_ref[:r, :inner], dh_ref[:r, inner:], False)

        return c

    lax.fori_loop(0, (tb_ref[1, e] + MOST - 1) // MOST, piece, 0)


def weight_grads(ta, tb, uo, sv, ud, w1, w3, w2):
    n_exp, hidden, inner = w1.shape
    width = ud.shape[1]
    wspec = lambda a, b: pl.BlockSpec((1, a, b), lambda e, t, s: (e, 0, 0))
    hbm = pl.BlockSpec(memory_space=pl.ANY)
    most = MOST * UNIT
    spec = pltpu.PrefetchScalarGridSpec(
        num_scalar_prefetch=2,
        grid=(n_exp,),
        in_specs=[hbm, hbm, hbm, wspec(hidden, inner), wspec(hidden, inner), wspec(inner, hidden)],
        out_specs=[wspec(hidden, inner), wspec(hidden, inner), wspec(inner, hidden)],
        scratch_shapes=[
            pltpu.VMEM((2, most, width), BF16),
            pltpu.VMEM((2, most, 3 * inner), BF16),
            pltpu.VMEM((2, most, width), BF16),
            pltpu.VMEM((most, inner), BF16),
            pltpu.VMEM((most, 2 * inner), BF16),
            pltpu.SMEM((2,), I32),
            pltpu.SemaphoreType.DMA((2,)),
            pltpu.SemaphoreType.DMA((2,)),
            pltpu.SemaphoreType.DMA((2,)),
        ],
    )
    return pl.pallas_call(
        functools.partial(grads_kernel, n_exp=n_exp, hidden=hidden, inner=inner),
        out_shape=[jax.ShapeDtypeStruct(w.shape, F32) for w in (w1, w3, w2)],
        grid_spec=spec,
        name='weight_grads',
        cost_estimate=pl.CostEstimate(flops=90_000_000_000, bytes_accessed=150_000_000, transcendentals=4_000_000),
    )(ta, tb, uo, sv, ud, w1, w3, w2)


def combine_kernel(meta_ref, code_ref, g_ref, start_ref, r_ref_a, r_ref_b, o_ref, *rest, n_exp, hidden, which, more):
    if more:
        add_ref, keep_ref, go_ref, dg_ref, p_ref, slot_ref, buf_ref, hot_ref, gate_ref, sem_ref = rest
    else:
        p_ref, dg_ref, slot_ref, buf_ref, hot_ref, gate_ref, sem_ref = rest
    i = pl.program_id(0)

    def rel(k):
        return which[0] + k * (which[1] - which[0])

    def pull(k, s):
        def one(q, c):
            code = code_ref[rel(k), q]
            src = pl.multiple_of(code - lax.rem(code, GRP), GRP)
            pltpu.make_async_copy(o_ref.at[pl.ds(src, GRP), :], buf_ref.at[s, pl.ds(pl.multiple_of(q * GRP, GRP), GRP), :], sem_ref.at[s]).start()
            return c

        lax.fori_loop(0, meta_ref[rel(k)], one, 0)

    @pl.when(i == 0)
    def _():
        pull(0, 0)
        pull(1, 1)
        _slots(g_ref, start_ref, slot_ref)

    n_grp = meta_ref[rel(i)]
    n_step = (n_grp + PER - 1) // PER

    def blank(q, c):
        buf_ref[i, pl.ds(pl.multiple_of(q * GRP, GRP), GRP), :] = jnp.zeros((GRP, buf_ref.shape[2]), BF16)
        return c

    lax.fori_loop(n_grp, n_step * PER, blank, 0)
    if more:
        p_ref[...] = add_ref[...]
    else:
        p_ref[...] = jnp.zeros_like(p_ref)
    dg_ref[...] = jnp.zeros_like(dg_ref)

    def whole(q, c):
        pltpu.make_async_copy(o_ref.at[pl.ds(0, STEP), :], buf_ref.at[0, pl.ds(0, STEP), :], sem_ref.at[i]).wait()
        return c

    def single(q, c):
        pltpu.make_async_copy(o_ref.at[pl.ds(0, GRP), :], buf_ref.at[0, pl.ds(0, GRP), :], sem_ref.at[i]).wait()
        return c

    lax.fori_loop(0, n_grp // PER, whole, 0)
    lax.fori_loop(0, lax.rem(n_grp, PER), single, 0)

    def step(k, c):
        rows = pl.ds(pl.multiple_of(k * STEP, STEP), STEP)
        o = buf_ref[i, rows, :hidden]
        rg = buf_ref[i, rows, hidden:]
        prod = _dot(o, jnp.where(i == 0, r_ref_a[...], r_ref_b[...]), 1, 1)
        _onehot(code_ref, rel(i), k, slot_ref, g_ref, hot_ref, gate_ref, n_exp)
        hot = hot_ref[...]
        prod = jnp.where(hot.astype(F32) > 0.5, prod, 0.0)
        for q in range(PER):
            e = lax.rem(code_ref[rel(i), k * PER + q], GRP)
            dg_ref[0, pl.ds(e, 1), :] += jnp.sum(prod[q * GRP : (q + 1) * GRP, :], axis=0, keepdims=True)
        gsel = gate_ref[...]
        g_hi = gsel.astype(BF16)
        rest = gsel - g_hi.astype(F32)
        g_mid = rest.astype(BF16)
        g_lo = (rest - g_mid.astype(F32)).astype(BF16)
        p_ref[:, :hidden] += _dot(g_hi, o, 0, 0) + (_dot(g_mid, o, 0, 0) + _dot(g_lo, o, 0, 0))
        p_ref[:, hidden:] += _dot(hot, rg, 0, 0)
        return c

    lax.fori_loop(0, n_step, step, 0)
    if more:

        @pl.when(i == 0)
        def _():
            keep_ref[...] = p_ref[...]

        @pl.when(i == 1)
        def _():
            go_ref[...] = p_ref[...]


def combine(meta, code, gates, start, blocks, o_rows, which, n_exp, add=None):
    width = o_rows.shape[1]
    hidden = width // 2
    half = pl.BlockSpec((BLK, hidden), lambda i, m, s: (0, 1))
    block = pl.BlockSpec((BLK, width), lambda i, m, s: (i, 0))
    more = [] if add is None else [add]
    whole = pl.BlockSpec(gates.shape, lambda i, m, s: (0, 0))
    fixed = pl.BlockSpec((BLK, width), lambda i, m, s: (0, 0))
    spec = pltpu.PrefetchScalarGridSpec(
        num_scalar_prefetch=2,
        grid=(2,),
        in_specs=[
            whole,
            whole,
            half,
            half,
            pl.BlockSpec(memory_space=pl.ANY),
            *([block] * len(more)),
        ],
        out_specs=([fixed] * 2 if more else [block]) + [pl.BlockSpec((1, n_exp, BLK), lambda i, m, s: (i, 0, 0))],
        scratch_shapes=[
            *([pltpu.VMEM((BLK, width), F32)] * len(more)),
            pltpu.VMEM(gates.shape, I32),
            pltpu.VMEM((2, BLK * n_exp, width), BF16),
            pltpu.VMEM((STEP, BLK), BF16),
            pltpu.VMEM((STEP, BLK), F32),
            pltpu.SemaphoreType.DMA((2,)),
        ],
    )
    return pl.pallas_call(
        functools.partial(combine_kernel, n_exp=n_exp, hidden=hidden, which=which, more=bool(more)),
        out_shape=([jax.ShapeDtypeStruct((BLK, width), F32)] * 2 if more else [jax.ShapeDtypeStruct((2 * BLK, width), F32)]) + [jax.ShapeDtypeStruct((2, n_exp, BLK), F32)],
        grid_spec=spec,
        name='combine',
        cost_estimate=pl.CostEstimate(flops=8_000_000_000, bytes_accessed=20_000_000, transcendentals=0),
    )(meta, code, gates, start, blocks[which[0]], blocks[which[1]], o_rows, *more)


def routing_tables(cnt, n_own):
    n_blk, n_exp = cnt.shape
    pad = (cnt + GRP - 1) // GRP * GRP
    before_e = (jnp.arange(n_exp)[:, None] < jnp.arange(n_exp)[None, :]).astype(I32)
    blk = jnp.arange(n_blk)
    same = (blk[:, None] < n_own) == (blk[None, :] < n_own)
    before_b = ((blk[:, None] < blk[None, :]) & same).astype(I32)
    blk_start = jnp.sum(pad[:, :, None] * before_e[None], axis=1)
    blk_end = blk_start + pad
    in_exp = jnp.sum(pad[:, None, :] * before_b[:, :, None], axis=0)

    def part(p):
        total = jnp.sum(p, axis=0)
        units = jnp.maximum((total + UNIT - 1) // UNIT, 1)
        first = jnp.sum(units[:, None] * before_e, axis=0)
        zero = jnp.stack([(first * UNIT + total) // GRP, (units * UNIT - total) // GRP])
        return jnp.stack([first, units]).astype(I32), zero.astype(I32), first * UNIT

    ta, za, base_a = part(pad[:n_own])
    tb, zb, base_b = part(pad[n_own:])
    base = jnp.where(blk[:, None] < n_own, base_a[None], base_b[None])
    q = jnp.arange(BLK * n_exp // GRP, dtype=I32) * GRP
    inside = (q[None, :, None] >= blk_start[:, None, :]) & (q[None, :, None] < blk_end[:, None, :])
    place = base + in_exp - blk_start + jnp.arange(n_exp, dtype=I32)[None]
    code = jnp.sum(jnp.where(inside, place[:, None, :] + q[None, :, None], 0), axis=2)
    start = jnp.broadcast_to(blk_start.reshape(n_blk * n_exp, 1), (n_blk * n_exp, BLK)).astype(I32)
    return (jnp.sum(pad, axis=1) // GRP).astype(I32), start, code.astype(I32), ta, za, tb, zb


def solution(mesh):
    ep_size = mesh.shape['ep']
    dp_size = mesh.shape['dp']
    n_dev = ep_size * dp_size
    all_axes = ('dp', 'ep')

    def swap(v, mask):
        return lax.ppermute(v, all_axes, [(d, d ^ mask) for d in range(n_dev)])

    def layer(tokens, w_router, w_gate, w_up, w_down, top_ids, r_proj):
        n_local, hidden = tokens.shape
        local_exp = w_gate.shape[0]
        xr = jnp.concatenate([tokens, r_proj], axis=1)
        blk = {0: xr}
        own_gates, gates, *got = first_stage(tokens, w_router.T, top_ids.T, xr, n_dev, ep_size)
        blk.update(zip((1, 2, 4, 8, 3, 5, 9), got))
        for dst, src, mask in ((6, 4, 2), (12, 8, 4), (10, 2, 8)):
            blk[dst] = swap(blk[src], mask)
        cnt = jnp.sum((gates >= 0).astype(I32), axis=2)
        gates = gates.reshape(n_dev * local_exp, n_local)
        meta, start, code, ta, za, tb, zb = routing_tables(cnt, ep_size)
        own_n = ep_size * n_local * local_exp + local_exp * UNIT
        oth_n = (n_dev - ep_size) * n_local * local_exp + local_exp * UNIT
        uo = sort_rows(meta, code, za, gates, start, blk, (0, 1, 2, 3), own_n, local_exp)
        o_rows, sv = own_rows(ta, uo, w_gate, w_up, w_down)
        o_rows, blk[6], blk[10], blk[12] = lax.optimization_barrier((o_rows, blk[6], blk[10], blk[12]))
        blk[14] = swap(blk[12], 2)
        for k in (6, 10, 12):
            blk[k + 1] = swap(blk[k], 1)
        ud = sort_rows(meta, code, zb, gates, start, blk, (4, 5, 8, 9, 6, 10, 12), oth_n, local_exp)
        p_send, dg_b = combine(meta, code, gates, start, blk, o_rows, (1, 3), local_exp)
        blk[15] = swap(blk[14], 1)
        p_sib = swap(p_send, 1)
        ud = sort_rows(meta, code, jnp.zeros_like(zb), gates, start, blk, (7, 11, 13, 14, 15), oth_n, local_exp, ud)
        p_sib, ud = lax.optimization_barrier((p_sib, ud))
        p_keep, p_go, dg_a = combine(meta, code, gates, start, blk, o_rows, (0, 2), local_exp, p_sib)
        dg = jnp.stack([dg_a[0], dg_b[0], dg_a[1], dg_b[1]])
        dz_t, grad_router_t = router_backward(dg, own_gates, tokens, n_dev, ep_size)
        p_go, dz_t = lax.optimization_barrier((p_go, dz_t))
        p_far = swap(p_go, 2)
        g_gate, g_up, g_down = weight_grads(ta, tb, uo, sv, ud, w_gate, w_up, w_down)
        grad_router = grad_router_t.T
        y = tokens.astype(F32) + (p_keep[:, :hidden] + p_far[:, :hidden])
        dx = r_proj.astype(F32) + _dot(dz_t, w_router, 0, 1) + (p_keep[:, hidden:] + p_far[:, hidden:])
        return y, dx, g_gate, g_up, g_down, grad_router

    tok_spec = P(all_axes, None)
    exp_spec = P('ep', None, None)
    return jax.shard_map(layer, mesh=mesh, in_specs=(tok_spec, P(), exp_spec, exp_spec, exp_spec, tok_spec, tok_spec), out_specs=(tok_spec, tok_spec, exp_spec, exp_spec, exp_spec, P()), check_vma=False)
```
